128 devices in a mesh: grp: 2 (over core), dp: 64 (over y, x, z).
Axes of the slice: x: 4, y: 4, z: 4, core: 2. Of those that a mesh axis runs over, the one named last changes fastest.
Arguments:
- grad: bfloat16 [2, 32768, 8192], P('grp', None, 'dp'), may hold values from -40 to 40
- residual: bfloat16 [2, 32768, 8192], P('grp', None, 'dp'), may hold values from -4 to 4
- q_prev: float32 [5, 4, 8192], P(None, None, 'dp'), may hold values from -0.0625 to 0.0625
- owner_table: int32 [5], replicated, may hold values from 0 to 63, as said below
Outputs:
- new_residual: bfloat16 [2, 32768, 8192], P('grp', None, 'dp')
- q_new: float32 [5, 4, 8192], P(None, None, 'dp')
- owned: float32 [64, 4, 14336], P('dp')
The draws below stay inside these ranges and needn't reach their ends.
Inputs may be any that keep to these rules, and one draw needn't show every extreme that they name: `owner_table`: the 5 owners are distinct.
All inputs are finite; a program needn't handle non-finite values.
Results may differ from the reference program's by a relative error of at most 0.0055.
Values sent between devices are 32-bit elements; how exact they have to be, the bound alone decides.
No kernel may reach another device: no remote copies, remote signals or barrier semaphores. Data moves between devices by JAX's collectives and lax.ppermute only.
A program may use at most 128 MiB of HBM per device.

```python
import jax
import jax.numpy as jnp
from jax import lax

D = 8192
KV = 1024
FF_WIN = 14336
LAYERS = 5
RANK = 4
R_ALL = 32768
CAP = 14336
N_GRP = 2
N_DP = 64


def draw_grad(key, part):
    shared = jax.random.normal(jax.random.fold_in(key, 11), (R_ALL, D), jnp.float32)
    private_part = jax.random.normal(jax.random.fold_in(key, 12), (N_GRP, R_ALL, D), jnp.float32)
    values = 0.3 * shared[None] + 0.95 * private_part
    return jnp.clip(values, -40.0, 40.0).astype(jnp.bfloat16)


def draw_owner_table(key, part):
    middle = jax.random.permutation(jax.random.fold_in(key, 21), N_DP - 2)[:LAYERS - 2].astype(jnp.int32) + 1
    ends = jnp.array([0, N_DP - 1], jnp.int32)
    table = jnp.concatenate([ends, middle])
    order = jax.random.permutation(jax.random.fold_in(key, 22), LAYERS)
    return table[order].astype(jnp.int32)


def steps_of(stream_key, dims, cuts, least, high):
    gain, own = 1.0, jax.random.fold_in(stream_key, 6)
    for axis_at, shards_of in cuts:
        draws = jnp.exp(jax.random.uniform(jax.random.fold_in(own, axis_at), (shards_of,), jnp.float32, least / len(cuts), high / len(cuts)))
        gain = gain * jnp.repeat(draws, dims[axis_at] // shards_of).reshape([-1 if axis == axis_at else 1 for axis in range(len(dims))])
    return gain


def bell_draw(key, shape, scale, limit, cuts=(), kind=jnp.bfloat16):
    drawn = jax.random.normal(key, shape, jnp.float32) * scale
    if len(cuts) > 0:
        drawn = steps_of(key, shape, cuts, -0.22, 0.18) * drawn
    return jnp.clip(drawn, min=-limit, max=limit).astype(kind)


def setup_inputs(seed: int = 0) -> dict:
    streams_of = jax.random.split(jax.random.key(seed), 5)
    grad = draw_grad(jax.random.fold_in(streams_of[4], 71), 0)
    residual = bell_draw(streams_of[1], (N_GRP, R_ALL, D), 0.5, 4.0, ((0, 2), (2, 64)))
    q_prev = bell_draw(streams_of[2], (LAYERS, RANK, D), D ** -0.5, 0.0625, ((2, 64),), jnp.float32)
    owner_table = draw_owner_table(jax.random.fold_in(streams_of[4], 71), 0)
    return {"grad": grad, "residual": residual, "q_prev": q_prev, "owner_table": owner_table}


EPSILON = 1e-06

def block_sizes():
    return [D, KV, KV, D, FF_WIN]

def whiten(lower_factor, projected):
    solved = []
    for i in range(projected.shape[-2]):
        running = projected[..., i, :]
        for k in range(i):
            running = running - lower_factor[..., i, k, None] * solved[k]
        solved.append(running / lower_factor[..., i, i, None])
    return jnp.stack(solved, axis=-2)

def orthonormal(projected):
    gram_matrix = jnp.dot(projected, projected.T, precision=lax.Precision.HIGHEST)
    gram_matrix = gram_matrix + EPSILON * jnp.eye(projected.shape[0], dtype=jnp.float32)
    return whiten(jnp.linalg.cholesky(gram_matrix), projected)

def reference(grad, residual, q_prev, owner_table):
    owned = jnp.zeros((N_DP, RANK, CAP), jnp.float32)
    residuals = []
    q_list = []
    offset = 0
    for layer_id, count in enumerate(block_sizes()):
        compensated = (grad[:, offset:offset + count].astype(jnp.float32) + residual[:, offset:offset + count].astype(jnp.float32)).astype(jnp.bfloat16)
        q_rounded = q_prev[layer_id].astype(jnp.bfloat16)
        projected = jnp.zeros((RANK, count), jnp.float32)
        for group in range(N_GRP):
            projected = projected + lax.dot_general(q_rounded.astype(jnp.float32), compensated[group].astype(jnp.float32), (((1,), (1,)), ((), ())), preferred_element_type=jnp.float32)
        projected = projected / N_GRP
        padded = jnp.pad(projected, ((0, 0), (0, CAP - count)))
        owned = lax.dynamic_update_slice(owned, padded[None], (owner_table[layer_id], jnp.int32(0), jnp.int32(0)))
        basis_rounded = orthonormal(projected).astype(jnp.bfloat16)
        q_sum = jnp.zeros((RANK, D), jnp.float32)
        for group in range(N_GRP):
            q_sum = q_sum + jnp.dot(basis_rounded.astype(jnp.float32), compensated[group].astype(jnp.float32), preferred_element_type=jnp.float32)
        q_new = q_sum / N_GRP
        q_round = q_new.astype(jnp.bfloat16)
        update = lax.dot_general(basis_rounded.astype(jnp.float32), q_round.astype(jnp.float32), (((0,), (0,)), ((), ())), preferred_element_type=jnp.float32)
        residuals.append((compensated.astype(jnp.float32) - update[None]).astype(jnp.bfloat16))
        q_list.append(q_new)
        offset += count
    return (jnp.concatenate(residuals, axis=1), jnp.stack(q_list), owned)
```

```python
import functools

import jax
import jax.numpy as jnp
from jax import lax
from jax.experimental import pallas as pl
from jax.experimental.pallas import tpu as pltpu
from jax.sharding import PartitionSpec as P

D = 8192
KV = 1024
FF_WIN = 14336
SIZES = (D, KV, KV, D, FF_WIN)
ROWS = sum(SIZES)
LANES = 128
TILE = 512
HALF = TILE // 2
TILES = ROWS // TILE
GROUP = 8
EPSILON = 1e-06
SWAP = ((0, 1), (1, 0))
F32, BF16 = jnp.float32, jnp.bfloat16
MIB = 1 << 20


def tile_layers():
    return [layer for layer, rows in enumerate(SIZES) for _ in range(rows // TILE)]


def layer_starts():
    starts, at = [], 0
    for rows in SIZES:
        starts.append(at)
        at += rows // TILE
    return starts


VM = pl.BlockSpec(memory_space=pltpu.VMEM)
SM = pl.BlockSpec(memory_space=pltpu.SMEM)
HB = pl.BlockSpec(memory_space=pl.ANY)


CHUNK_TILES = 4
CHUNK = CHUNK_TILES * TILE
CHUNKS = ROWS // CHUNK


def project_kernel(g_ref, grad, residual, q_ref, comp_ref, keep_ref, send_ref, gbuf, rbuf, lhs, sems):
    def copies(c):
        rows = pl.ds(c * CHUNK, CHUNK)
        return (
            pltpu.make_async_copy(grad.at[0, rows], gbuf.at[rows], sems.at[0, c]),
            pltpu.make_async_copy(residual.at[0, rows], rbuf.at[rows], sems.at[1, c]),
        )

    for c in range(CHUNKS):
        for copy in copies(c):
            copy.start()
    own = g_ref[0]
    for layer in range(len(SIZES)):
        q = q_ref[layer].astype(BF16).astype(F32)
        zero = jnp.zeros_like(q)
        straight = jnp.concatenate(
            [jnp.concatenate([q, zero], 1), jnp.concatenate([zero, q], 1)], 0
        )
        crossed = jnp.concatenate(
            [jnp.concatenate([zero, q], 1), jnp.concatenate([q, zero], 1)], 0
        )
        lhs[layer] = jnp.where(own == 0, straight, crossed)

    def chunk(c, layers):
        for copy in copies(c):
            copy.wait()
        for k in range(CHUNK_TILES):
            t = c * CHUNK_TILES + k
            halves = []
            for h in range(2):
                rows = pl.ds(pl.multiple_of(t * TILE + h * HALF, HALF), HALF)
                value = (gbuf[rows].astype(F32) + rbuf[rows].astype(F32)).astype(BF16)
                comp_ref[rows] = value
                halves.append(value)
            out = lax.dot_general(
                lhs[layers[k]].astype(BF16),
                jnp.concatenate(halves, 1),
                (((1,), (1,)), ((), ())),
                preferred_element_type=F32,
            )
            keep_ref[t] = out[:4]
            send_ref[t] = out[4:]

    layers = tile_layers()
    groups = [tuple(layers[c * CHUNK_TILES : (c + 1) * CHUNK_TILES]) for c in range(CHUNKS)]
    c = 0
    while c < CHUNKS:
        end = c
        while end < CHUNKS and groups[end] == groups[c]:
            end += 1
        if end - c == 1:
            chunk(c, groups[c])
        else:
            lax.fori_loop(c, end, lambda i, _, now=groups[c]: chunk(i, now), None)
        c = end


def project(own, grad, residual, q_prev):
    share = jax.ShapeDtypeStruct((TILES, 4, HALF), F32)
    return pl.pallas_call(
        project_kernel,
        out_shape=(pltpu.VMEM((ROWS, LANES), BF16), share, share),
        in_specs=[SM, HB, HB, VM],
        out_specs=(VM, VM, VM),
        scratch_shapes=[
            pltpu.VMEM((ROWS, LANES), BF16),
            pltpu.VMEM((ROWS, LANES), BF16),
            pltpu.VMEM((len(SIZES), 8, 2 * LANES), F32),
            pltpu.SemaphoreType.DMA((2, CHUNKS)),
        ],
        compiler_params=pltpu.CompilerParams(vmem_limit_bytes=30 * MIB),
        name="project",
    )(own, grad, residual, q_prev)


def spread_kernel(x_ref, o_ref):
    total = x_ref[0]
    for i in range(1, TILES):
        total = total + x_ref[i]
    total = total * 0.5
    for i in range(TILES):
        o_ref[i] = total


def spread(x):
    return pl.pallas_call(
        spread_kernel,
        out_shape=jax.ShapeDtypeStruct((TILES, 4, HALF), F32),
        in_specs=[VM],
        out_specs=VM,
        compiler_params=pltpu.CompilerParams(vmem_limit_bytes=2 * MIB),
        name="spread",
    )(x)


def lane_sum(x):
    return jnp.sum(x, axis=1, keepdims=True)


def coefficients(grams):
    lane = lax.broadcasted_iota(jnp.int32, (8, LANES), 1)
    row = lax.broadcasted_iota(jnp.int32, (8, LANES), 0) % 4
    entry = {}
    for k in range(4):
        packed = jnp.zeros((8, LANES), F32)
        for layer, sums in enumerate(grams):
            s = sums[k][:, :LANES] + sums[k][:, LANES:]
            s = s + pltpu.roll(s, 4, 0)
            packed = jnp.where(lane == layer, lane_sum(s), packed)
        for i in range(k, 4):
            value = jnp.broadcast_to(packed[i : i + 1], (8, LANES))
            entry[i, i - k] = value + EPSILON if k == 0 else value
    g = entry
    i0 = lax.rsqrt(g[0, 0])
    l10, l20, l30 = g[1, 0] * i0, g[2, 0] * i0, g[3, 0] * i0
    i1 = lax.rsqrt(g[1, 1] - l10 * l10)
    l21 = (g[2, 1] - l20 * l10) * i1
    l31 = (g[3, 1] - l30 * l10) * i1
    i2 = lax.rsqrt(g[2, 2] - l20 * l20 - l21 * l21)
    l32 = (g[3, 2] - l30 * l20 - l31 * l21) * i2
    i3 = lax.rsqrt(g[3, 3] - l30 * l30 - l31 * l31 - l32 * l32)
    x = {(0, 0): i0, (1, 1): i1, (2, 2): i2, (3, 3): i3}
    x[1, 0] = -(l10 * i0) * i1
    x[2, 1] = -(l21 * i1) * i2
    x[3, 2] = -(l32 * i2) * i3
    x[2, 0] = -(l20 * i0 + l21 * x[1, 0]) * i2
    x[3, 1] = -(l31 * i1 + l32 * x[2, 1]) * i3
    x[3, 0] = -(l30 * i0 + l31 * x[1, 0] + l32 * x[2, 0]) * i3
    columns = []
    for k in range(4):
        packed = jnp.zeros((8, LANES), F32)
        for i in range(k, 4):
            packed = jnp.where(row == i, x[i, i - k], packed)
        columns.append(
            [
                jnp.broadcast_to(packed[:, layer : layer + 1], (8, 2 * LANES))
                for layer in range(len(SIZES))
            ]
        )
    return columns


def basis_kernel(g_ref, mine, other, comp, owned_hbm, q_ref, turned_ref, joined, stacked, owned, sem):
    own, place = g_ref[0], g_ref[1]
    counts = [rows // TILE for rows in SIZES]
    starts = layer_starts()

    owned[...] = jnp.zeros_like(owned)
    for layer, count in enumerate(counts):

        @pl.when(g_ref[2 + layer] == place)
        def _():
            def step(k, _):
                at = pl.multiple_of(k * TILE + own * HALF, HALF)
                owned[0, :, pl.ds(at, HALF)] = mine[starts[layer] + k]
                at = pl.multiple_of(k * TILE + (1 - own) * HALF, HALF)
                owned[0, :, pl.ds(at, HALF)] = other[starts[layer] + k]

            lax.fori_loop(0, count, step, None)

    copy = pltpu.make_async_copy(owned, owned_hbm, sem)
    copy.start()

    grams = []
    for layer, count in enumerate(counts):
        sums = [None] * 4
        for t in range(starts[layer], starts[layer] + count):
            v = jnp.concatenate([mine[t], other[t]], 0)
            joined[t] = v
            for k in range(4):
                term = v * (pltpu.roll(v, k, 0) if k else v)
                sums[k] = term if sums[k] is None else sums[k] + term
        grams.append(sums)
    columns = coefficients(grams)

    for layer, count in enumerate(counts):
        total = None
        for t in range(starts[layer], starts[layer] + count):
            v = joined[t]
            basis = v * columns[0][layer]
            for k in range(1, 4):
                basis = basis + pltpu.roll(v, k, 0) * columns[k][layer]
            rounded = basis.astype(BF16)
            back = rounded.astype(F32)
            at = (t % GROUP) * 16
            stacked[t // GROUP, at : at + 8] = back[:, :LANES]
            stacked[t // GROUP, at + 8 : at + 16] = back[:, LANES:]
            first = comp[pl.ds(pl.multiple_of(t * TILE + own * HALF, HALF), HALF)]
            second = comp[pl.ds(pl.multiple_of(t * TILE + (1 - own) * HALF, HALF), HALF)]
            part = jnp.dot(
                rounded, jnp.concatenate([first, second], 1), preferred_element_type=F32
            )
            total = part if total is None else total + part
        q_ref[layer] = total[:4, :LANES] + total[4:, LANES:]
    for n in range(TILES // GROUP):
        turned_ref[n] = stacked[n].T.astype(BF16)
    copy.wait()


def orthonormal_bases(scalars, mine, other, comp):
    return pl.pallas_call(
        basis_kernel,
        out_shape=(
            jax.ShapeDtypeStruct((1, 4, max(SIZES)), F32),
            jax.ShapeDtypeStruct((len(SIZES), 4, LANES), F32),
            pltpu.VMEM((TILES // GROUP, LANES, LANES), BF16),
        ),
        in_specs=[SM, VM, VM, VM],
        out_specs=(HB, VM, VM),
        scratch_shapes=[
            pltpu.VMEM((TILES, 8, HALF), F32),
            pltpu.VMEM((TILES // GROUP, LANES, LANES), F32),
            pltpu.VMEM((1, 4, max(SIZES)), F32),
            pltpu.SemaphoreType.DMA,
        ],
        compiler_params=pltpu.CompilerParams(vmem_limit_bytes=16 * MIB),
        name="bases",
    )(scalars, mine, other, comp)


def residual_kernel(g_ref, q_mine, q_other, turned, comp, out_hbm, q_ref, weights, obuf, sems):
    own = g_ref[0]
    layers = tile_layers()
    q_new = (q_mine[...] + q_other[...]) * 0.5
    q_ref[...] = q_new
    rounded = q_new.astype(BF16).astype(F32)
    weights[...] = jnp.zeros_like(weights)
    groups = TILES // GROUP
    for n in range(groups):
        for c in range(2 * GROUP):
            q = rounded[layers[n * GROUP + c // 2]]
            h = c % 2
            weights[n, c * 8 : c * 8 + 8, h * LANES : (h + 1) * LANES] = jnp.concatenate([q, q], 0)
    lane = lax.broadcasted_iota(jnp.int32, (LANES, LANES), 1)

    def copy(n):
        rows = pl.ds(n * GROUP * TILE, GROUP * TILE)
        return pltpu.make_async_copy(obuf.at[rows], out_hbm.at[0, rows], sems.at[n])

    def group(n, _):
        w = weights[n].astype(BF16)
        left = turned[n]
        for k in range(GROUP):
            for other in range(2):
                chosen = (lane // 16 == k) & ((lane // 4) % 2 == other)
                update = jnp.dot(
                    jnp.where(chosen, left, jnp.zeros_like(left)), w, preferred_element_type=F32
                )
                which = own if other == 0 else 1 - own
                at = pl.multiple_of((n * GROUP + k) * TILE + which * HALF, HALF)
                for h in range(2):
                    rows = pl.ds(pl.multiple_of(at + h * LANES, LANES), LANES)
                    obuf[rows] = (
                        comp[rows].astype(F32) - update[:, h * LANES : (h + 1) * LANES]
                    ).astype(BF16)
        copy(n).start()

    lax.fori_loop(0, groups, group, None)
    for n in range(groups):
        copy(n).wait()


def new_residual(scalars, q_mine, q_other, turned, comp):
    return pl.pallas_call(
        residual_kernel,
        out_shape=(
            jax.ShapeDtypeStruct((1, ROWS, LANES), BF16),
            jax.ShapeDtypeStruct((len(SIZES), 4, LANES), F32),
        ),
        in_specs=[SM, VM, VM, VM, VM],
        out_specs=(HB, VM),
        scratch_shapes=[
            pltpu.VMEM((TILES // GROUP, LANES, 2 * LANES), F32),
            pltpu.VMEM((ROWS, LANES), BF16),
            pltpu.SemaphoreType.DMA((TILES // GROUP,)),
        ],
        compiler_params=pltpu.CompilerParams(vmem_limit_bytes=24 * MIB),
        name="new_residual",
    )(scalars, q_mine, q_other, turned, comp)


def body(grad, residual, q_prev, owner_table):
    own = lax.axis_index("grp").astype(jnp.int32)
    place = lax.axis_index("dp").astype(jnp.int32)
    scalars = jnp.concatenate([jnp.stack([own, place]), owner_table])
    comp, keep, send = project(scalars, grad, residual, q_prev)
    both = keep + lax.ppermute(send, "grp", SWAP)
    arrived = lax.all_to_all(both, "dp", 0, 0, tiled=True)
    mine = lax.all_to_all(spread(arrived), "dp", 0, 0, tiled=True)
    other = lax.ppermute(mine, "grp", SWAP)
    owned, q_part, turned = orthonormal_bases(scalars, mine, other, comp)
    q_there = lax.ppermute(q_part, "grp", SWAP)
    out, q_new = new_residual(scalars, q_part, q_there, turned, comp)
    return out, q_new, owned


def solution(mesh):
    in_specs = (P("grp", None, "dp"), P("grp", None, "dp"), P(None, None, "dp"), P())
    out_specs = (P("grp", None, "dp"), P(None, None, "dp"), P("dp", None, None))
    return jax.shard_map(body, mesh=mesh, in_specs=in_specs, out_specs=out_specs, check_vma=False)
```

```python
import functools

import jax
import jax.numpy as jnp
from jax import lax
from jax.experimental import pallas as pl
from jax.experimental.pallas import tpu as pltpu
from jax.sharding import PartitionSpec as P

D = 8192
KV = 1024
FF_WIN = 14336
SIZES = (D, KV, KV, D, FF_WIN)
ROWS = sum(SIZES)
LANES = 128
TILE = 512
HALF = TILE // 2
TILES = ROWS // TILE
GROUP = 8
EPSILON = 1e-06
SWAP = ((0, 1), (1, 0))
F32, BF16 = jnp.float32, jnp.bfloat16
MIB = 1 << 20


def tile_layers():
    return [layer for layer, rows in enumerate(SIZES) for _ in range(rows // TILE)]


def layer_starts():
    starts, at = [], 0
    for rows in SIZES:
        starts.append(at)
        at += rows // TILE
    return starts


VM = pl.BlockSpec(memory_space=pltpu.VMEM)
SM = pl.BlockSpec(memory_space=pltpu.SMEM)
HB = pl.BlockSpec(memory_space=pltpu.HBM)


CHUNK_TILES = 4
CHUNK = CHUNK_TILES * TILE
CHUNKS = ROWS // CHUNK


def project_kernel(grad, residual, q_hbm, comp_ref, keep_ref, send_ref, gbuf, rbuf, q_ref, lhs, sems, q_sem):
    def copies(c):
        rows = pl.ds(c * CHUNK, CHUNK)
        return (
            pltpu.make_async_copy(grad.at[0, rows], gbuf.at[rows], sems.at[0, c]),
            pltpu.make_async_copy(residual.at[0, rows], rbuf.at[rows], sems.at[1, c]),
        )

    q_copy = pltpu.make_async_copy(q_hbm, q_ref, q_sem)
    q_copy.start()
    for c in range(CHUNKS):
        for copy in copies(c):
            copy.start()
    own = lax.axis_index("grp")
    q_copy.wait()
    for layer in range(len(SIZES)):
        q = q_ref[layer].astype(BF16).astype(F32)
        zero = jnp.zeros_like(q)
        straight = jnp.concatenate(
            [jnp.concatenate([q, zero], 1), jnp.concatenate([zero, q], 1)], 0
        )
        crossed = jnp.concatenate(
            [jnp.concatenate([zero, q], 1), jnp.concatenate([q, zero], 1)], 0
        )
        lhs[layer] = jnp.where(own == 0, straight, crossed)

    def chunk(c, layers):
        for copy in copies(c):
            copy.wait()
        for k in range(CHUNK_TILES):
            t = c * CHUNK_TILES + k
            halves = []
            for h in range(2):
                rows = pl.ds(pl.multiple_of(t * TILE + h * HALF, HALF), HALF)
                value = (gbuf[rows].astype(F32) + rbuf[rows].astype(F32)).astype(BF16)
                comp_ref[rows] = value
                halves.append(value)
            out = lax.dot_general(
                lhs[layers[k]].astype(BF16),
                jnp.concatenate(halves, 1),
                (((1,), (1,)), ((), ())),
                preferred_element_type=F32,
            )
            keep_ref[t] = out[:4]
            send_ref[t] = out[4:]

    layers = tile_layers()
    groups = [tuple(layers[c * CHUNK_TILES : (c + 1) * CHUNK_TILES]) for c in range(CHUNKS)]
    c = 0
    while c < CHUNKS:
        end = c
        while end < CHUNKS and groups[end] == groups[c]:
            end += 1
        if end - c == 1:
            chunk(c, groups[c])
        else:
            lax.fori_loop(c, end, lambda i, _, now=groups[c]: chunk(i, now), None)
        c = end


def project(grad, residual, q_prev):
    share = jax.ShapeDtypeStruct((TILES, 4, HALF), F32)
    return pl.pallas_call(
        project_kernel,
        out_shape=(pltpu.VMEM((ROWS, LANES), BF16), share, share),
        in_specs=[HB, HB, HB],
        out_specs=(VM, VM, VM),
        scratch_shapes=[
            pltpu.VMEM((ROWS, LANES), BF16),
            pltpu.VMEM((ROWS, LANES), BF16),
            pltpu.VMEM((len(SIZES), 4, LANES), F32),
            pltpu.VMEM((len(SIZES), 8, 2 * LANES), F32),
            pltpu.SemaphoreType.DMA((2, CHUNKS)),
            pltpu.SemaphoreType.DMA,
        ],
        compiler_params=pltpu.CompilerParams(vmem_limit_bytes=30 * MIB),
        name="project",
    )(*(pltpu.with_memory_space_constraint(x, pltpu.HBM) for x in (grad, residual, q_prev)))


def spread_kernel(x_ref, o_ref):
    total = x_ref[0]
    for i in range(1, TILES):
        total = total + x_ref[i]
    total = total * 0.5
    for i in range(TILES):
        o_ref[i] = total


def spread(x):
    return pl.pallas_call(
        spread_kernel,
        out_shape=jax.ShapeDtypeStruct((TILES, 4, HALF), F32),
        in_specs=[VM],
        out_specs=VM,
        compiler_params=pltpu.CompilerParams(vmem_limit_bytes=2 * MIB),
        name="spread",
    )(x)


def lane_sum(x):
    return jnp.sum(x, axis=1, keepdims=True)


def coefficients(grams):
    lane = lax.broadcasted_iota(jnp.int32, (8, LANES), 1)
    row = lax.broadcasted_iota(jnp.int32, (8, LANES), 0) % 4
    entry = {}
    for k in range(4):
        packed = jnp.zeros((8, LANES), F32)
        for layer, sums in enumerate(grams):
            s = sums[k][:, :LANES] + sums[k][:, LANES:]
            s = s + pltpu.roll(s, 4, 0)
            packed = jnp.where(lane == layer, lane_sum(s), packed)
        for i in range(k, 4):
            value = jnp.broadcast_to(packed[i : i + 1], (8, LANES))
            entry[i, i - k] = value + EPSILON if k == 0 else value
    g = entry
    i0 = lax.rsqrt(g[0, 0])
    l10, l20, l30 = g[1, 0] * i0, g[2, 0] * i0, g[3, 0] * i0
    i1 = lax.rsqrt(g[1, 1] - l10 * l10)
    l21 = (g[2, 1] - l20 * l10) * i1
    l31 = (g[3, 1] - l30 * l10) * i1
    i2 = lax.rsqrt(g[2, 2] - l20 * l20 - l21 * l21)
    l32 = (g[3, 2] - l30 * l20 - l31 * l21) * i2
    i3 = lax.rsqrt(g[3, 3] - l30 * l30 - l31 * l31 - l32 * l32)
    x = {(0, 0): i0, (1, 1): i1, (2, 2): i2, (3, 3): i3}
    x[1, 0] = -(l10 * i0) * i1
    x[2, 1] = -(l21 * i1) * i2
    x[3, 2] = -(l32 * i2) * i3
    x[2, 0] = -(l20 * i0 + l21 * x[1, 0]) * i2
    x[3, 1] = -(l31 * i1 + l32 * x[2, 1]) * i3
    x[3, 0] = -(l30 * i0 + l31 * x[1, 0] + l32 * x[2, 0]) * i3
    columns = []
    for k in range(4):
        packed = jnp.zeros((8, LANES), F32)
        for i in range(k, 4):
            packed = jnp.where(row == i, x[i, i - k], packed)
        columns.append(
            [
                jnp.broadcast_to(packed[:, layer : layer + 1], (8, 2 * LANES))
                for layer in range(len(SIZES))
            ]
        )
    return columns


def basis_kernel(owner, mine, other, comp, owned_hbm, q_ref, turned_ref, joined, stacked, owned, sem):
    own, place = lax.axis_index("grp"), lax.axis_index("dp")
    counts = [rows // TILE for rows in SIZES]
    starts = layer_starts()

    owned[...] = jnp.zeros_like(owned)
    for layer, count in enumerate(counts):

        @pl.when(owner[layer] == place)
        def _():
            def step(k, _):
                at = pl.multiple_of(k * TILE + own * HALF, HALF)
                owned[0, :, pl.ds(at, HALF)] = mine[starts[layer] + k]
                at = pl.multiple_of(k * TILE + (1 - own) * HALF, HALF)
                owned[0, :, pl.ds(at, HALF)] = other[starts[layer] + k]

            lax.fori_loop(0, count, step, None)

    copy = pltpu.make_async_copy(owned, owned_hbm, sem)
    copy.start()

    grams = []
    for layer, count in enumerate(counts):
        sums = [None] * 4
        for t in range(starts[layer], starts[layer] + count):
            v = jnp.concatenate([mine[t], other[t]], 0)
            joined[t] = v
            for k in range(4):
                term = v * (pltpu.roll(v, k, 0) if k else v)
                sums[k] = term if sums[k] is None else sums[k] + term
        grams.append(sums)
    columns = coefficients(grams)

    for layer, count in enumerate(counts):
        total = None
        for t in range(starts[layer], starts[layer] + count):
            v = joined[t]
            basis = v * columns[0][layer]
            for k in range(1, 4):
                basis = basis + pltpu.roll(v, k, 0) * columns[k][layer]
            rounded = basis.astype(BF16)
            back = rounded.astype(F32)
            at = (t % GROUP) * 16
            stacked[t // GROUP, at : at + 8] = back[:, :LANES]
            stacked[t // GROUP, at + 8 : at + 16] = back[:, LANES:]
            first = comp[pl.ds(pl.multiple_of(t * TILE + own * HALF, HALF), HALF)]
            second = comp[pl.ds(pl.multiple_of(t * TILE + (1 - own) * HALF, HALF), HALF)]
            part = jnp.dot(
                rounded, jnp.concatenate([first, second], 1), preferred_element_type=F32
            )
            total = part if total is None else total + part
        q_ref[layer] = total[:4, :LANES] + total[4:, LANES:]
    for n in range(TILES // GROUP):
        turned_ref[n] = stacked[n].T.astype(BF16)
    copy.wait()


def orthonormal_bases(owner_table, mine, other, comp):
    return pl.pallas_call(
        basis_kernel,
        out_shape=(
            jax.ShapeDtypeStruct((1, 4, max(SIZES)), F32),
            jax.ShapeDtypeStruct((len(SIZES), 4, LANES), F32),
            pltpu.VMEM((TILES // GROUP, LANES, LANES), BF16),
        ),
        in_specs=[SM, VM, VM, VM],
        out_specs=(HB, VM, VM),
        scratch_shapes=[
            pltpu.VMEM((TILES, 8, HALF), F32),
            pltpu.VMEM((TILES // GROUP, LANES, LANES), F32),
            pltpu.VMEM((1, 4, max(SIZES)), F32),
            pltpu.SemaphoreType.DMA,
        ],
        compiler_params=pltpu.CompilerParams(vmem_limit_bytes=16 * MIB),
        name="bases",
    )(owner_table, mine, other, comp)


PIECE = 4
PIECES = TILES // PIECE


def residual_kernel(q_mine, q_other, turned, comp, out_hbm, q_ref, weights, obuf, sems):
    own = lax.axis_index("grp")
    layers = tile_layers()
    q_new = (q_mine[...] + q_other[...]) * 0.5
    q_ref[...] = q_new
    rounded = q_new.astype(BF16).astype(F32)
    zero = jnp.zeros((4, LANES), F32)
    for layer in range(len(SIZES)):
        q = rounded[layer]
        rows = (jnp.concatenate([q, zero], 1), jnp.concatenate([zero, q], 1))
        none = jnp.zeros((4, 2 * LANES), F32)
        weights[layer, 0] = jnp.concatenate([rows[0], none, rows[1], none], 0)
        weights[layer, 1] = jnp.concatenate([none, rows[0], none, rows[1]], 0)

    def copy(n):
        rows = pl.ds(n * PIECE * TILE, PIECE * TILE)
        return pltpu.make_async_copy(obuf.at[rows], out_hbm.at[0, rows], sems.at[n])

    for n in range(TILES // GROUP):
        left = turned[n]
        for k in range(GROUP):
            t = n * GROUP + k
            for other in range(2):
                w = weights[layers[t], other].astype(BF16)
                parts = [w]
                if k:
                    parts.insert(0, jnp.zeros((16 * k, 2 * LANES), BF16))
                if k < GROUP - 1:
                    parts.append(jnp.zeros((LANES - 16 * (k + 1), 2 * LANES), BF16))
                update = jnp.dot(left, jnp.concatenate(parts, 0), preferred_element_type=F32)
                which = own if other == 0 else 1 - own
                at = pl.multiple_of(t * TILE + which * HALF, HALF)
                for h in range(2):
                    rows = pl.ds(pl.multiple_of(at + h * LANES, LANES), LANES)
                    obuf[rows] = (
                        comp[rows].astype(F32) - update[:, h * LANES : (h + 1) * LANES]
                    ).astype(BF16)
            if t % PIECE == PIECE - 1:
                copy(t // PIECE).start()
    for n in range(PIECES):
        copy(n).wait()


def new_residual(q_mine, q_other, turned, comp):
    return pl.pallas_call(
        residual_kernel,
        out_shape=(
            jax.ShapeDtypeStruct((1, ROWS, LANES), BF16),
            jax.ShapeDtypeStruct((len(SIZES), 4, LANES), F32),
        ),
        in_specs=[VM, VM, VM, VM],
        out_specs=(HB, VM),
        scratch_shapes=[
            pltpu.VMEM((len(SIZES), 2, 16, 2 * LANES), F32),
            pltpu.VMEM((ROWS, LANES), BF16),
            pltpu.SemaphoreType.DMA((PIECES,)),
        ],
        compiler_params=pltpu.CompilerParams(vmem_limit_bytes=24 * MIB),
        name="new_residual",
    )(q_mine, q_other, turned, comp)


def body(grad, residual, q_prev, owner_table):
    comp, keep, send = project(grad, residual, q_prev)
    both = keep + lax.ppermute(send, "grp", SWAP)
    arrived = lax.all_to_all(both, "dp", 0, 0, tiled=True)
    mine = lax.all_to_all(spread(arrived), "dp", 0, 0, tiled=True)
    other = lax.ppermute(mine, "grp", SWAP)
    owned, q_part, turned = orthonormal_bases(owner_table, mine, other, comp)
    q_there = lax.ppermute(q_part, "grp", SWAP)
    out, q_new = new_residual(q_part, q_there, turned, comp)
    return out, q_new, owned


def solution(mesh):
    in_specs = (P("grp", None, "dp"), P("grp", None, "dp"), P(None, None, "dp"), P())
    out_specs = (P("grp", None, "dp"), P(None, None, "dp"), P("dp", None, None))
    return jax.shard_map(body, mesh=mesh, in_specs=in_specs, out_specs=out_specs, check_vma=False)
```

```python
import functools

import jax
import jax.numpy as jnp
from jax import lax
from jax.experimental import pallas as pl
from jax.experimental.pallas import tpu as pltpu
from jax.sharding import PartitionSpec as P

D = 8192
KV = 1024
FF_WIN = 14336
SIZES = (D, KV, KV, D, FF_WIN)
ROWS = sum(SIZES)
LANES = 128
TILE = 512
HALF = TILE // 2
TILES = ROWS // TILE
GROUP = 8
EPSILON = 1e-06
SWAP = ((0, 1), (1, 0))
F32, BF16 = jnp.float32, jnp.bfloat16
MIB = 1 << 20


def tile_layers():
    return [layer for layer, rows in enumerate(SIZES) for _ in range(rows // TILE)]


def layer_starts():
    starts, at = [], 0
    for rows in SIZES:
        starts.append(at)
        at += rows // TILE
    return starts


VM = pl.BlockSpec(memory_space=pltpu.VMEM)
SM = pl.BlockSpec(memory_space=pltpu.SMEM)
HB = pl.BlockSpec(memory_space=pltpu.HBM)


CHUNKS = (16, 16, 16, 8, 4, 4)
DEPTH = 3


def project_kernel(grad, residual, q_hbm, comp_ref, keep_ref, send_ref, gbuf, rbuf, q_ref, lhs, sems, q_sem):
    firsts = [sum(CHUNKS[:c]) for c in range(len(CHUNKS))]

    def copies(c):
        rows = pl.ds(firsts[c] * TILE, CHUNKS[c] * TILE)
        return (
            pltpu.make_async_copy(grad.at[0, rows], gbuf.at[rows], sems.at[0, c]),
            pltpu.make_async_copy(residual.at[0, rows], rbuf.at[rows], sems.at[1, c]),
        )

    q_copy = pltpu.make_async_copy(q_hbm, q_ref, q_sem)
    q_copy.start()
    for c in range(DEPTH):
        for copy in copies(c):
            copy.start()
    own = lax.axis_index("grp")
    q_copy.wait()
    for layer in range(len(SIZES)):
        q = q_ref[layer].astype(BF16).astype(F32)
        zero = jnp.zeros_like(q)
        straight = jnp.concatenate(
            [jnp.concatenate([q, zero], 1), jnp.concatenate([zero, q], 1)], 0
        )
        crossed = jnp.concatenate(
            [jnp.concatenate([zero, q], 1), jnp.concatenate([q, zero], 1)], 0
        )
        lhs[layer] = jnp.where(own == 0, straight, crossed)

    layers = tile_layers()
    for c, count in enumerate(CHUNKS):
        for copy in copies(c):
            copy.wait()
        if c + DEPTH < len(CHUNKS):
            for copy in copies(c + DEPTH):
                copy.start()
        for t in range(firsts[c], firsts[c] + count):
            halves = []
            for h in range(2):
                rows = slice(t * TILE + h * HALF, t * TILE + (h + 1) * HALF)
                value = (gbuf[rows].astype(F32) + rbuf[rows].astype(F32)).astype(BF16)
                comp_ref[rows] = value
                halves.append(value)
            out = lax.dot_general(
                lhs[layers[t]].astype(BF16),
                jnp.concatenate(halves, 1),
                (((1,), (1,)), ((), ())),
                preferred_element_type=F32,
            )
            keep_ref[t] = out[:4]
            send_ref[t] = out[4:]


def project(grad, residual, q_prev):
    share = jax.ShapeDtypeStruct((TILES, 4, HALF), F32)
    return pl.pallas_call(
        project_kernel,
        out_shape=(pltpu.VMEM((ROWS, LANES), BF16), share, share),
        in_specs=[HB, HB, HB],
        out_specs=(VM, VM, VM),
        scratch_shapes=[
            pltpu.VMEM((ROWS, LANES), BF16),
            pltpu.VMEM((ROWS, LANES), BF16),
            pltpu.VMEM((len(SIZES), 4, LANES), F32),
            pltpu.VMEM((len(SIZES), 8, 2 * LANES), F32),
            pltpu.SemaphoreType.DMA((2, len(CHUNKS))),
            pltpu.SemaphoreType.DMA,
        ],
        compiler_params=pltpu.CompilerParams(vmem_limit_bytes=30 * MIB),
        name="project",
    )(*(pltpu.with_memory_space_constraint(x, pltpu.HBM) for x in (grad, residual, q_prev)))


def spread_kernel(x_ref, o_ref):
    total = x_ref[0]
    for i in range(1, TILES):
        total = total + x_ref[i]
    total = total * 0.5
    for i in range(TILES):
        o_ref[i] = total


def spread(x):
    return pl.pallas_call(
        spread_kernel,
        out_shape=jax.ShapeDtypeStruct((TILES, 4, HALF), F32),
        in_specs=[VM],
        out_specs=VM,
        compiler_params=pltpu.CompilerParams(vmem_limit_bytes=2 * MIB),
        name="spread",
    )(x)


def lane_sum(x):
    return jnp.sum(x, axis=1, keepdims=True)


def coefficients(grams):
    lane = lax.broadcasted_iota(jnp.int32, (8, LANES), 1)
    row = lax.broadcasted_iota(jnp.int32, (8, LANES), 0) % 4
    entry = {}
    for k in range(4):
        packed = jnp.zeros((8, LANES), F32)
        for layer, sums in enumerate(grams):
            s = sums[k][:, :LANES] + sums[k][:, LANES:]
            s = s + pltpu.roll(s, 4, 0)
            packed = jnp.where(lane == layer, lane_sum(s), packed)
        for i in range(k, 4):
            value = jnp.broadcast_to(packed[i : i + 1], (8, LANES))
            entry[i, i - k] = value + EPSILON if k == 0 else value
    g = entry
    i0 = lax.rsqrt(g[0, 0])
    l10, l20, l30 = g[1, 0] * i0, g[2, 0] * i0, g[3, 0] * i0
    i1 = lax.rsqrt(g[1, 1] - l10 * l10)
    l21 = (g[2, 1] - l20 * l10) * i1
    l31 = (g[3, 1] - l30 * l10) * i1
    i2 = lax.rsqrt(g[2, 2] - l20 * l20 - l21 * l21)
    l32 = (g[3, 2] - l30 * l20 - l31 * l21) * i2
    i3 = lax.rsqrt(g[3, 3] - l30 * l30 - l31 * l31 - l32 * l32)
    x = {(0, 0): i0, (1, 1): i1, (2, 2): i2, (3, 3): i3}
    x[1, 0] = -(l10 * i0) * i1
    x[2, 1] = -(l21 * i1) * i2
    x[3, 2] = -(l32 * i2) * i3
    x[2, 0] = -(l20 * i0 + l21 * x[1, 0]) * i2
    x[3, 1] = -(l31 * i1 + l32 * x[2, 1]) * i3
    x[3, 0] = -(l30 * i0 + l31 * x[1, 0] + l32 * x[2, 0]) * i3
    columns = []
    for k in range(4):
        packed = jnp.zeros((8, LANES), F32)
        for i in range(k, 4):
            packed = jnp.where(row == i, x[i, i - k], packed)
        columns.append(
            [
                jnp.broadcast_to(packed[:, layer : layer + 1], (8, 2 * LANES))
                for layer in range(len(SIZES))
            ]
        )
    return columns


def basis_kernel(mine, other, comp, q_ref, turned_ref, joined, stacked):
    own = lax.axis_index("grp")
    counts = [rows // TILE for rows in SIZES]
    starts = layer_starts()

    grams = []
    for layer, count in enumerate(counts):
        sums = [None] * 4
        for t in range(starts[layer], starts[layer] + count):
            v = jnp.concatenate([mine[t], other[t]], 0)
            joined[t] = v
            for k in range(4):
                term = v * (pltpu.roll(v, k, 0) if k else v)
                sums[k] = term if sums[k] is None else sums[k] + term
        grams.append(sums)
    columns = coefficients(grams)

    for layer, count in enumerate(counts):
        total = None
        for t in range(starts[layer], starts[layer] + count):
            v = joined[t]
            basis = v * columns[0][layer]
            for k in range(1, 4):
                basis = basis + pltpu.roll(v, k, 0) * columns[k][layer]
            rounded = basis.astype(BF16)
            back = rounded.astype(F32)
            at = (t % GROUP) * 16
            stacked[t // GROUP, at : at + 8] = back[:, :LANES]
            stacked[t // GROUP, at + 8 : at + 16] = back[:, LANES:]
            first = comp[pl.ds(pl.multiple_of(t * TILE + own * HALF, HALF), HALF)]
            second = comp[pl.ds(pl.multiple_of(t * TILE + (1 - own) * HALF, HALF), HALF)]
            part = jnp.dot(
                rounded, jnp.concatenate([first, second], 1), preferred_element_type=F32
            )
            total = part if total is None else total + part
        q_ref[layer] = total[:4, :LANES] + total[4:, LANES:]
    for n in range(TILES // GROUP):
        turned_ref[n] = stacked[n].T.astype(BF16)


def orthonormal_bases(mine, other, comp):
    return pl.pallas_call(
        basis_kernel,
        out_shape=(
            jax.ShapeDtypeStruct((len(SIZES), 4, LANES), F32),
            pltpu.VMEM((TILES // GROUP, LANES, LANES), BF16),
        ),
        in_specs=[VM, VM, VM],
        out_specs=(VM, VM),
        scratch_shapes=[
            pltpu.VMEM((TILES, 8, HALF), F32),
            pltpu.VMEM((TILES // GROUP, LANES, LANES), F32),
        ],
        compiler_params=pltpu.CompilerParams(vmem_limit_bytes=16 * MIB),
        name="bases",
    )(mine, other, comp)


PIECE = 4
PIECES = TILES // PIECE


def residual_kernel(
    owner, q_mine, q_other, turned, comp, mine, other_half, out_hbm, q_ref, owned_hbm, weights, obuf, owned, sems
):
    own, place = lax.axis_index("grp"), lax.axis_index("dp")
    owned_copy = pltpu.make_async_copy(owned, owned_hbm, sems.at[PIECES])

    def write_owned():
        owned[...] = jnp.zeros_like(owned)
        for layer, first in enumerate(layer_starts()):

            @pl.when(owner[layer] == place)
            def _():
                def step(k, _):
                    at = pl.multiple_of(k * TILE + own * HALF, HALF)
                    owned[0, :, pl.ds(at, HALF)] = mine[first + k]
                    at = pl.multiple_of(k * TILE + (1 - own) * HALF, HALF)
                    owned[0, :, pl.ds(at, HALF)] = other_half[first + k]

                lax.fori_loop(0, SIZES[layer] // TILE, step, None)

        owned_copy.start()

    layers = tile_layers()
    q_new = (q_mine[...] + q_other[...]) * 0.5
    q_ref[...] = q_new
    rounded = q_new.astype(BF16).astype(F32)
    zero = jnp.zeros((4, LANES), F32)
    for layer in range(len(SIZES)):
        q = rounded[layer]
        rows = (jnp.concatenate([q, zero], 1), jnp.concatenate([zero, q], 1))
        none = jnp.zeros((4, 2 * LANES), F32)
        weights[layer, 0] = jnp.concatenate([rows[0], none, rows[1], none], 0)
        weights[layer, 1] = jnp.concatenate([none, rows[0], none, rows[1]], 0)

    def copy(n):
        rows = pl.ds(n * PIECE * TILE, PIECE * TILE)
        return pltpu.make_async_copy(obuf.at[rows], out_hbm.at[0, rows], sems.at[n])

    for n in range(TILES // GROUP):
        left = turned[n]
        for k in range(GROUP):
            t = n * GROUP + k
            for other in range(2):
                w = weights[layers[t], other].astype(BF16)
                parts = [w]
                if k:
                    parts.insert(0, jnp.zeros((16 * k, 2 * LANES), BF16))
                if k < GROUP - 1:
                    parts.append(jnp.zeros((LANES - 16 * (k + 1), 2 * LANES), BF16))
                update = jnp.dot(left, jnp.concatenate(parts, 0), preferred_element_type=F32)
                which = own if other == 0 else 1 - own
                at = pl.multiple_of(t * TILE + which * HALF, HALF)
                for h in range(2):
                    rows = pl.ds(pl.multiple_of(at + h * LANES, LANES), LANES)
                    obuf[rows] = (
                        comp[rows].astype(F32) - update[:, h * LANES : (h + 1) * LANES]
                    ).astype(BF16)
            if t % PIECE == PIECE - 1:
                copy(t // PIECE).start()
        if n == 1:
            write_owned()
    owned_copy.wait()
    for n in range(PIECES):
        copy(n).wait()


def new_residual(owner_table, q_mine, q_other, turned, comp, mine, other):
    return pl.pallas_call(
        residual_kernel,
        out_shape=(
            jax.ShapeDtypeStruct((1, ROWS, LANES), BF16),
            jax.ShapeDtypeStruct((len(SIZES), 4, LANES), F32),
            jax.ShapeDtypeStruct((1, 4, max(SIZES)), F32),
        ),
        in_specs=[SM, VM, VM, VM, VM, VM, VM],
        out_specs=(HB, VM, HB),
        scratch_shapes=[
            pltpu.VMEM((len(SIZES), 2, 16, 2 * LANES), F32),
            pltpu.VMEM((ROWS, LANES), BF16),
            pltpu.VMEM((1, 4, max(SIZES)), F32),
            pltpu.SemaphoreType.DMA((PIECES + 1,)),
        ],
        compiler_params=pltpu.CompilerParams(vmem_limit_bytes=24 * MIB),
        name="new_residual",
    )(owner_table, q_mine, q_other, turned, comp, mine, other)


def body(grad, residual, q_prev, owner_table):
    comp, keep, send = project(grad, residual, q_prev)
    both = keep + lax.ppermute(send, "grp", SWAP)
    arrived = lax.all_to_all(both, "dp", 0, 0, tiled=True)
    mine = lax.all_to_all(spread(arrived), "dp", 0, 0, tiled=True)
    other = lax.ppermute(mine, "grp", SWAP)
    q_part, turned = orthonormal_bases(mine, other, comp)
    q_there = lax.ppermute(q_part, "grp", SWAP)
    return new_residual(owner_table, q_part, q_there, turned, comp, mine, other)


def solution(mesh):
    in_specs = (P("grp", None, "dp"), P("grp", None, "dp"), P(None, None, "dp"), P())
    out_specs = (P("grp", None, "dp"), P(None, None, "dp"), P("dp", None, None))
    return jax.shard_map(body, mesh=mesh, in_specs=in_specs, out_specs=out_specs, check_vma=False)
```

```python
import functools

import jax
import jax.numpy as jnp
from jax import lax
from jax.experimental import pallas as pl
from jax.experimental.pallas import tpu as pltpu
from jax.sharding import PartitionSpec as P

D = 8192
KV = 1024
FF_WIN = 14336
SIZES = (D, KV, KV, D, FF_WIN)
ROWS = sum(SIZES)
LANES = 128
TILE = 512
HALF = TILE // 2
TILES = ROWS // TILE
GROUP = 8
EPSILON = 1e-06
SWAP = ((0, 1), (1, 0))
F32, BF16 = jnp.float32, jnp.bfloat16
MIB = 1 << 20


def tile_layers():
    return [layer for layer, rows in enumerate(SIZES) for _ in range(rows // TILE)]


def layer_starts():
    starts, at = [], 0
    for rows in SIZES:
        starts.append(at)
        at += rows // TILE
    return starts


VM = pl.BlockSpec(memory_space=pltpu.VMEM)
HB = pl.BlockSpec(memory_space=pltpu.HBM)


CHUNKS = (8, 16, 24, 8, 4, 4)
DEPTH = 3


def project_kernel(grad, residual, q_hbm, comp_ref, keep_ref, send_ref, gbuf, rbuf, q_ref, lhs, sems, q_sem):
    firsts = [sum(CHUNKS[:c]) for c in range(len(CHUNKS))]

    def copies(c):
        rows = pl.ds(firsts[c] * TILE, CHUNKS[c] * TILE)
        return (
            pltpu.make_async_copy(grad.at[0, rows], gbuf.at[rows], sems.at[0, c]),
            pltpu.make_async_copy(residual.at[0, rows], rbuf.at[rows], sems.at[1, c]),
        )

    q_copy = pltpu.make_async_copy(q_hbm, q_ref, q_sem)
    q_copy.start()
    for c in range(DEPTH):
        for copy in copies(c):
            copy.start()
    own = lax.axis_index("grp")
    q_copy.wait()
    for layer in range(len(SIZES)):
        q = q_ref[layer].astype(BF16).astype(F32)
        zero = jnp.zeros_like(q)
        straight = jnp.concatenate(
            [jnp.concatenate([q, zero], 1), jnp.concatenate([zero, q], 1)], 0
        )
        crossed = jnp.concatenate(
            [jnp.concatenate([zero, q], 1), jnp.concatenate([q, zero], 1)], 0
        )
        lhs[layer] = jnp.where(own == 0, straight, crossed)

    layers = tile_layers()
    for c, count in enumerate(CHUNKS):
        for copy in copies(c):
            copy.wait()
        if c + DEPTH < len(CHUNKS):
            for copy in copies(c + DEPTH):
                copy.start()
        for t in range(firsts[c], firsts[c] + count):
            halves = []
            for h in range(2):
                rows = slice(t * TILE + h * HALF, t * TILE + (h + 1) * HALF)
                value = (gbuf[rows].astype(F32) + rbuf[rows].astype(F32)).astype(BF16)
                comp_ref[rows] = value
                halves.append(value)
            out = lax.dot_general(
                lhs[layers[t]].astype(BF16),
                jnp.concatenate(halves, 1),
                (((1,), (1,)), ((), ())),
                preferred_element_type=F32,
            )
            keep_ref[t] = out[:4]
            send_ref[t] = out[4:]


def project(grad, residual, q_prev):
    share = jax.ShapeDtypeStruct((TILES, 4, HALF), F32)
    return pl.pallas_call(
        project_kernel,
        out_shape=(pltpu.VMEM((ROWS, LANES), BF16), share, share),
        in_specs=[HB, HB, HB],
        out_specs=(VM, VM, VM),
        scratch_shapes=[
            pltpu.VMEM((ROWS, LANES), BF16),
            pltpu.VMEM((ROWS, LANES), BF16),
            pltpu.VMEM((len(SIZES), 4, LANES), F32),
            pltpu.VMEM((len(SIZES), 8, 2 * LANES), F32),
            pltpu.SemaphoreType.DMA((2, len(CHUNKS))),
            pltpu.SemaphoreType.DMA,
        ],
        compiler_params=pltpu.CompilerParams(vmem_limit_bytes=30 * MIB),
        name="project",
    )(*(pltpu.with_memory_space_constraint(x, pltpu.HBM) for x in (grad, residual, q_prev)))


def spread_kernel(x_ref, o_ref):
    total = x_ref[0]
    for i in range(1, TILES):
        total = total + x_ref[i]
    total = total * 0.5
    for i in range(TILES):
        o_ref[i] = total


def spread(x):
    return pl.pallas_call(
        spread_kernel,
        out_shape=jax.ShapeDtypeStruct((TILES, 4, HALF), F32),
        in_specs=[VM],
        out_specs=VM,
        compiler_params=pltpu.CompilerParams(vmem_limit_bytes=2 * MIB),
        name="spread",
    )(x)


def lane_sum(x):
    return jnp.sum(x, axis=1, keepdims=True)


def coefficients(grams):
    lane = lax.broadcasted_iota(jnp.int32, (8, LANES), 1)
    row = lax.broadcasted_iota(jnp.int32, (8, LANES), 0) % 4
    entry = {}
    for k in range(4):
        packed = jnp.zeros((8, LANES), F32)
        for layer, sums in enumerate(grams):
            s = sums[k][:, :LANES] + sums[k][:, LANES:]
            s = s + pltpu.roll(s, 4, 0)
            packed = jnp.where(lane == layer, lane_sum(s), packed)
        for i in range(k, 4):
            value = jnp.broadcast_to(packed[i : i + 1], (8, LANES))
            entry[i, i - k] = value + EPSILON if k == 0 else value
    g = entry
    i0 = lax.rsqrt(g[0, 0])
    l10, l20, l30 = g[1, 0] * i0, g[2, 0] * i0, g[3, 0] * i0
    i1 = lax.rsqrt(g[1, 1] - l10 * l10)
    l21 = (g[2, 1] - l20 * l10) * i1
    l31 = (g[3, 1] - l30 * l10) * i1
    i2 = lax.rsqrt(g[2, 2] - l20 * l20 - l21 * l21)
    l32 = (g[3, 2] - l30 * l20 - l31 * l21) * i2
    i3 = lax.rsqrt(g[3, 3] - l30 * l30 - l31 * l31 - l32 * l32)
    x = {(0, 0): i0, (1, 1): i1, (2, 2): i2, (3, 3): i3}
    x[1, 0] = -(l10 * i0) * i1
    x[2, 1] = -(l21 * i1) * i2
    x[3, 2] = -(l32 * i2) * i3
    x[2, 0] = -(l20 * i0 + l21 * x[1, 0]) * i2
    x[3, 1] = -(l31 * i1 + l32 * x[2, 1]) * i3
    x[3, 0] = -(l30 * i0 + l31 * x[1, 0] + l32 * x[2, 0]) * i3
    columns = []
    for k in range(4):
        packed = jnp.zeros((8, LANES), F32)
        for i in range(k, 4):
            packed = jnp.where(row == i, x[i, i - k], packed)
        columns.append(
            [
                jnp.broadcast_to(packed[:, layer : layer + 1], (8, 2 * LANES))
                for layer in range(len(SIZES))
            ]
        )
    return columns


def basis_kernel(mine, other, comp, q_ref, turned_ref, joined, stacked):
    own = lax.axis_index("grp")
    counts = [rows // TILE for rows in SIZES]
    starts = layer_starts()

    grams = []
    for layer, count in enumerate(counts):
        sums = [None] * 4
        for t in range(starts[layer], starts[layer] + count):
            v = jnp.concatenate([mine[t], other[t]], 0)
            joined[t] = v
            for k in range(4):
                term = v * (pltpu.roll(v, k, 0) if k else v)
                sums[k] = term if sums[k] is None else sums[k] + term
        grams.append(sums)
    columns = coefficients(grams)

    for layer, count in enumerate(counts):
        total = None
        for t in range(starts[layer], starts[layer] + count):
            v = joined[t]
            basis = v * columns[0][layer]
            for k in range(1, 4):
                basis = basis + pltpu.roll(v, k, 0) * columns[k][layer]
            rounded = basis.astype(BF16)
            back = rounded.astype(F32)
            at = (t % GROUP) * 16
            stacked[t // GROUP, at : at + 8] = back[:, :LANES]
            stacked[t // GROUP, at + 8 : at + 16] = back[:, LANES:]
            first = comp[pl.ds(pl.multiple_of(t * TILE + own * HALF, HALF), HALF)]
            second = comp[pl.ds(pl.multiple_of(t * TILE + (1 - own) * HALF, HALF), HALF)]
            part = jnp.dot(
                rounded, jnp.concatenate([first, second], 1), preferred_element_type=F32
            )
            total = part if total is None else total + part
        q_ref[layer] = total[:4, :LANES] + total[4:, LANES:]
    for n in range(TILES // GROUP):
        turned_ref[n] = stacked[n].T.astype(BF16)


def orthonormal_bases(mine, other, comp):
    return pl.pallas_call(
        basis_kernel,
        out_shape=(
            jax.ShapeDtypeStruct((len(SIZES), 4, LANES), F32),
            pltpu.VMEM((TILES // GROUP, LANES, LANES), BF16),
        ),
        in_specs=[VM, VM, VM],
        out_specs=(VM, VM),
        scratch_shapes=[
            pltpu.VMEM((TILES, 8, HALF), F32),
            pltpu.VMEM((TILES // GROUP, LANES, LANES), F32),
        ],
        compiler_params=pltpu.CompilerParams(vmem_limit_bytes=16 * MIB),
        name="bases",
    )(mine, other, comp)


PIECE = 4
PIECES = TILES // PIECE


def residual_kernel(
    owner_hbm, q_mine, q_other, turned, comp, mine, other_half,
    out_hbm, q_hbm, owned_hbm,
    weights, obuf, owned, q_ref, owner, sems,
):
    own, place = lax.axis_index("grp"), lax.axis_index("dp")
    owned_copy = pltpu.make_async_copy(owned, owned_hbm, sems.at[PIECES])
    q_copy = pltpu.make_async_copy(q_ref, q_hbm, sems.at[PIECES + 1])
    owner_copy = pltpu.make_async_copy(owner_hbm, owner, sems.at[PIECES + 2])
    owner_copy.start()

    def write_owned():
        owner_copy.wait()
        owned[...] = jnp.zeros_like(owned)
        for layer, first in enumerate(layer_starts()):

            @pl.when(owner[layer] == place)
            def _():
                def step(k, _):
                    at = pl.multiple_of(k * TILE + own * HALF, HALF)
                    owned[0, :, pl.ds(at, HALF)] = mine[first + k]
                    at = pl.multiple_of(k * TILE + (1 - own) * HALF, HALF)
                    owned[0, :, pl.ds(at, HALF)] = other_half[first + k]

                lax.fori_loop(0, SIZES[layer] // TILE, step, None)

        owned_copy.start()

    layers = tile_layers()
    q_new = (q_mine[...] + q_other[...]) * 0.5
    q_ref[...] = q_new
    q_copy.start()
    rounded = q_new.astype(BF16).astype(F32)
    zero = jnp.zeros((4, LANES), F32)
    for layer in range(len(SIZES)):
        q = rounded[layer]
        rows = (jnp.concatenate([q, zero], 1), jnp.concatenate([zero, q], 1))
        none = jnp.zeros((4, 2 * LANES), F32)
        weights[layer, 0] = jnp.concatenate([rows[0], none, rows[1], none], 0)
        weights[layer, 1] = jnp.concatenate([none, rows[0], none, rows[1]], 0)

    def copy(n):
        rows = pl.ds(n * PIECE * TILE, PIECE * TILE)
        return pltpu.make_async_copy(obuf.at[rows], out_hbm.at[0, rows], sems.at[n])

    for n in range(TILES // GROUP):
        left = turned[n]
        for k in range(GROUP):
            t = n * GROUP + k
            for other in range(2):
                w = weights[layers[t], other].astype(BF16)
                parts = [w]
                if k:
                    parts.insert(0, jnp.zeros((16 * k, 2 * LANES), BF16))
                if k < GROUP - 1:
                    parts.append(jnp.zeros((LANES - 16 * (k + 1), 2 * LANES), BF16))
                update = jnp.dot(left, jnp.concatenate(parts, 0), preferred_element_type=F32)
                which = own if other == 0 else 1 - own
                at = pl.multiple_of(t * TILE + which * HALF, HALF)
                for h in range(2):
                    rows = pl.ds(pl.multiple_of(at + h * LANES, LANES), LANES)
                    obuf[rows] = (
                        comp[rows].astype(F32) - update[:, h * LANES : (h + 1) * LANES]
                    ).astype(BF16)
            if t % PIECE == PIECE - 1:
                copy(t // PIECE).start()
        if n == TILES // GROUP - 1:
            write_owned()
    owned_copy.wait()
    q_copy.wait()
    for n in range(PIECES):
        copy(n).wait()


def new_residual(owner_table, q_mine, q_other, turned, comp, mine, other):
    return pl.pallas_call(
        residual_kernel,
        out_shape=(
            jax.ShapeDtypeStruct((1, ROWS, LANES), BF16),
            jax.ShapeDtypeStruct((len(SIZES), 4, LANES), F32),
            jax.ShapeDtypeStruct((1, 4, max(SIZES)), F32),
        ),
        in_specs=[HB, VM, VM, VM, VM, VM, VM],
        out_specs=(HB, HB, HB),
        scratch_shapes=[
            pltpu.VMEM((len(SIZES), 2, 16, 2 * LANES), F32),
            pltpu.VMEM((ROWS, LANES), BF16),
            pltpu.VMEM((1, 4, max(SIZES)), F32),
            pltpu.VMEM((len(SIZES), 4, LANES), F32),
            pltpu.SMEM((len(SIZES),), jnp.int32),
            pltpu.SemaphoreType.DMA((PIECES + 3,)),
        ],
        compiler_params=pltpu.CompilerParams(vmem_limit_bytes=24 * MIB),
        name="new_residual",
    )(
        pltpu.with_memory_space_constraint(owner_table, pltpu.HBM),
        q_mine, q_other, turned, comp, mine, other,
    )


def body(grad, residual, q_prev, owner_table):
    comp, keep, send = project(grad, residual, q_prev)
    both = keep + lax.ppermute(send, "grp", SWAP)
    arrived = lax.all_to_all(both, "dp", 0, 0, tiled=True)
    mine = lax.all_to_all(spread(arrived), "dp", 0, 0, tiled=True)
    other = lax.ppermute(mine, "grp", SWAP)
    q_part, turned = orthonormal_bases(mine, other, comp)
    q_there = lax.ppermute(q_part, "grp", SWAP)
    return new_residual(owner_table, q_part, q_there, turned, comp, mine, other)


def solution(mesh):
    in_specs = (P("grp", None, "dp"), P("grp", None, "dp"), P(None, None, "dp"), P())
    out_specs = (P("grp", None, "dp"), P(None, None, "dp"), P("dp", None, None))
    return jax.shard_map(body, mesh=mesh, in_specs=in_specs, out_specs=out_specs, check_vma=False)
```

```python
import functools

import jax
import jax.numpy as jnp
from jax import lax
from jax.experimental import pallas as pl
from jax.experimental.pallas import tpu as pltpu
from jax.sharding import PartitionSpec as P

D = 8192
KV = 1024
FF_WIN = 14336
SIZES = (D, KV, KV, D, FF_WIN)
ROWS = sum(SIZES)
LANES = 128
TILE = 512
HALF = TILE // 2
TILES = ROWS // TILE
GROUP = 8
EPSILON = 1e-06
SWAP = ((0, 1), (1, 0))
F32, BF16 = jnp.float32, jnp.bfloat16
MIB = 1 << 20


def tile_layers():
    return [layer for layer, rows in enumerate(SIZES) for _ in range(rows // TILE)]


def layer_starts():
    starts, at = [], 0
    for rows in SIZES:
        starts.append(at)
        at += rows // TILE
    return starts


VM = pl.BlockSpec(memory_space=pltpu.VMEM)
HB = pl.BlockSpec(memory_space=pltpu.HBM)


CHUNKS = (8, 16, 24, 8, 4, 4)
DEPTH = 3


def project_kernel(
    grad, residual, q_hbm, owner_hbm,
    comp_ref, keep_ref, send_ref, flags_ref,
    gbuf, rbuf, q_ref, lhs, owner, sems, q_sem, owner_sem,
):
    firsts = [sum(CHUNKS[:c]) for c in range(len(CHUNKS))]

    def copies(c):
        rows = pl.ds(firsts[c] * TILE, CHUNKS[c] * TILE)
        return (
            pltpu.make_async_copy(grad.at[0, rows], gbuf.at[rows], sems.at[0, c]),
            pltpu.make_async_copy(residual.at[0, rows], rbuf.at[rows], sems.at[1, c]),
        )

    q_copy = pltpu.make_async_copy(q_hbm, q_ref, q_sem)
    q_copy.start()
    owner_copy = pltpu.make_async_copy(owner_hbm, owner, owner_sem)
    owner_copy.start()
    for c in range(DEPTH):
        for copy in copies(c):
            copy.start()
    own = lax.axis_index("grp")
    q_copy.wait()
    for layer in range(len(SIZES)):
        q = q_ref[layer].astype(BF16).astype(F32)
        zero = jnp.zeros_like(q)
        straight = jnp.concatenate(
            [jnp.concatenate([q, zero], 1), jnp.concatenate([zero, q], 1)], 0
        )
        crossed = jnp.concatenate(
            [jnp.concatenate([zero, q], 1), jnp.concatenate([q, zero], 1)], 0
        )
        lhs[layer] = jnp.where(own == 0, straight, crossed)
    owner_copy.wait()
    place = lax.axis_index("dp")
    for layer in range(len(SIZES)):
        flags_ref[layer] = jnp.full((4, HALF), jnp.where(owner[layer] == place, 1.0, 0.0), F32)

    layers = tile_layers()
    for c, count in enumerate(CHUNKS):
        for copy in copies(c):
            copy.wait()
        if c + DEPTH < len(CHUNKS):
            for copy in copies(c + DEPTH):
                copy.start()
        for t in range(firsts[c], firsts[c] + count):
            halves = []
            for h in range(2):
                rows = slice(t * TILE + h * HALF, t * TILE + (h + 1) * HALF)
                value = (gbuf[rows].astype(F32) + rbuf[rows].astype(F32)).astype(BF16)
                comp_ref[rows] = value
                halves.append(value)
            out = lax.dot_general(
                lhs[layers[t]].astype(BF16),
                jnp.concatenate(halves, 1),
                (((1,), (1,)), ((), ())),
                preferred_element_type=F32,
            )
            keep_ref[t] = out[:4]
            send_ref[t] = out[4:]


def project(grad, residual, q_prev, owner_table):
    share = jax.ShapeDtypeStruct((TILES, 4, HALF), F32)
    return pl.pallas_call(
        project_kernel,
        out_shape=(
            pltpu.VMEM((ROWS, LANES), BF16),
            share,
            share,
            pltpu.VMEM((len(SIZES), 4, HALF), F32),
        ),
        in_specs=[HB, HB, HB, HB],
        out_specs=(VM, VM, VM, VM),
        scratch_shapes=[
            pltpu.VMEM((ROWS, LANES), BF16),
            pltpu.VMEM((ROWS, LANES), BF16),
            pltpu.VMEM((len(SIZES), 4, LANES), F32),
            pltpu.VMEM((len(SIZES), 8, 2 * LANES), F32),
            pltpu.SMEM((len(SIZES),), jnp.int32),
            pltpu.SemaphoreType.DMA((2, len(CHUNKS))),
            pltpu.SemaphoreType.DMA,
            pltpu.SemaphoreType.DMA,
        ],
        compiler_params=pltpu.CompilerParams(vmem_limit_bytes=30 * MIB),
        name="project",
    )(*(pltpu.with_memory_space_constraint(x, pltpu.HBM) for x in (grad, residual, q_prev, owner_table)))


def spread_kernel(x_ref, o_ref):
    total = x_ref[0]
    for i in range(1, TILES):
        total = total + x_ref[i]
    total = total * 0.5
    for i in range(TILES):
        o_ref[i] = total


def spread(x):
    return pl.pallas_call(
        spread_kernel,
        out_shape=jax.ShapeDtypeStruct((TILES, 4, HALF), F32),
        in_specs=[VM],
        out_specs=VM,
        compiler_params=pltpu.CompilerParams(vmem_limit_bytes=2 * MIB),
        name="spread",
    )(x)


def lane_sum(x):
    return jnp.sum(x, axis=1, keepdims=True)


def coefficients(grams):
    lane = lax.broadcasted_iota(jnp.int32, (8, LANES), 1)
    row = lax.broadcasted_iota(jnp.int32, (8, LANES), 0) % 4
    entry = {}
    for k in range(4):
        packed = jnp.zeros((8, LANES), F32)
        for layer, sums in enumerate(grams):
            s = sums[k][:, :LANES] + sums[k][:, LANES:]
            s = s + pltpu.roll(s, 4, 0)
            packed = jnp.where(lane == layer, lane_sum(s), packed)
        for i in range(k, 4):
            value = jnp.broadcast_to(packed[i : i + 1], (8, LANES))
            entry[i, i - k] = value + EPSILON if k == 0 else value
    g = entry
    i0 = lax.rsqrt(g[0, 0])
    l10, l20, l30 = g[1, 0] * i0, g[2, 0] * i0, g[3, 0] * i0
    i1 = lax.rsqrt(g[1, 1] - l10 * l10)
    l21 = (g[2, 1] - l20 * l10) * i1
    l31 = (g[3, 1] - l30 * l10) * i1
    i2 = lax.rsqrt(g[2, 2] - l20 * l20 - l21 * l21)
    l32 = (g[3, 2] - l30 * l20 - l31 * l21) * i2
    i3 = lax.rsqrt(g[3, 3] - l30 * l30 - l31 * l31 - l32 * l32)
    x = {(0, 0): i0, (1, 1): i1, (2, 2): i2, (3, 3): i3}
    x[1, 0] = -(l10 * i0) * i1
    x[2, 1] = -(l21 * i1) * i2
    x[3, 2] = -(l32 * i2) * i3
    x[2, 0] = -(l20 * i0 + l21 * x[1, 0]) * i2
    x[3, 1] = -(l31 * i1 + l32 * x[2, 1]) * i3
    x[3, 0] = -(l30 * i0 + l31 * x[1, 0] + l32 * x[2, 0]) * i3
    columns = []
    for k in range(4):
        packed = jnp.zeros((8, LANES), F32)
        for i in range(k, 4):
            packed = jnp.where(row == i, x[i, i - k], packed)
        columns.append(
            [
                jnp.broadcast_to(packed[:, layer : layer + 1], (8, 2 * LANES))
                for layer in range(len(grams))
            ]
        )
    return columns


EARLY, LATE = (0,), (4, 3, 1, 2)


def basis_kernel(mine, other, comp, q_ref, stacked, joined):
    own = lax.axis_index("grp")
    counts = [rows // TILE for rows in SIZES]
    starts = layer_starts()

    def gram(layer):
        sums = [None] * 4
        for t in range(starts[layer], starts[layer] + counts[layer]):
            v = jnp.concatenate([mine[t], other[t]], 0)
            joined[t] = v
            for k in range(4):
                term = v * (pltpu.roll(v, k, 0) if k else v)
                sums[k] = term if sums[k] is None else sums[k] + term
        return sums

    def apply(layer, columns):
        total = None
        for t in range(starts[layer], starts[layer] + counts[layer]):
            v = joined[t]
            basis = v * columns[0]
            for k in range(1, 4):
                basis = basis + pltpu.roll(v, k, 0) * columns[k]
            rounded = basis.astype(BF16)
            back = rounded.astype(F32)
            at = (t % GROUP) * 16
            stacked[t // GROUP, at : at + 8] = back[:, :LANES]
            stacked[t // GROUP, at + 8 : at + 16] = back[:, LANES:]
            first = comp[pl.ds(pl.multiple_of(t * TILE + own * HALF, HALF), HALF)]
            second = comp[pl.ds(pl.multiple_of(t * TILE + (1 - own) * HALF, HALF), HALF)]
            part = jnp.dot(
                rounded, jnp.concatenate([first, second], 1), preferred_element_type=F32
            )
            total = part if total is None else total + part
        q_ref[layer] = total[:4, :LANES] + total[4:, LANES:]

    early = coefficients([gram(layer) for layer in EARLY])
    late_grams = [gram(layer) for layer in LATE]
    for i, layer in enumerate(EARLY):
        apply(layer, [column[i] for column in early])
    late = coefficients(late_grams)
    for i, layer in enumerate(LATE):
        apply(layer, [column[i] for column in late])


def orthonormal_bases(mine, other, comp):
    return pl.pallas_call(
        basis_kernel,
        out_shape=(
            jax.ShapeDtypeStruct((len(SIZES), 4, LANES), F32),
            pltpu.VMEM((TILES // GROUP, LANES, LANES), F32),
        ),
        in_specs=[VM, VM, VM],
        out_specs=(VM, VM),
        scratch_shapes=[pltpu.VMEM((TILES, 8, HALF), F32)],
        compiler_params=pltpu.CompilerParams(vmem_limit_bytes=16 * MIB),
        name="bases",
    )(mine, other, comp)


def aside_kernel(flags, mine, other, stacked, turned_ref, owned_ref):
    own = lax.axis_index("grp")
    for n in range(TILES // GROUP):
        turned_ref[n] = stacked[n].T.astype(BF16)
    starts = layer_starts()
    counts = [rows // TILE for rows in SIZES]
    held = [flags[layer] > 0.5 for layer in range(len(SIZES))]
    for k in range(max(counts)):
        for ref, which in ((mine, own), (other, 1 - own)):
            value = jnp.zeros((4, HALF), F32)
            for layer, first in enumerate(starts):
                if k < counts[layer]:
                    value = jnp.where(held[layer], ref[first + k], value)
            owned_ref[0, :, pl.ds(pl.multiple_of(k * TILE + which * HALF, HALF), HALF)] = value


def aside(flags, mine, other, stacked):
    return pl.pallas_call(
        aside_kernel,
        out_shape=(
            pltpu.VMEM((TILES // GROUP, LANES, LANES), BF16),
            pltpu.VMEM((1, 4, max(SIZES)), F32),
        ),
        in_specs=[VM, VM, VM, VM],
        out_specs=(VM, VM),
        compiler_params=pltpu.CompilerParams(vmem_limit_bytes=4 * MIB),
        cost_estimate=pl.CostEstimate(flops=2_000_000, bytes_accessed=1_000_000, transcendentals=0),
        name="aside",
    )(flags, mine, other, stacked)


PIECES = (4,) * 16


def residual_kernel(q_mine, q_other, turned, comp, out_hbm, q_hbm, weights, obuf, q_ref, sems):
    own = lax.axis_index("grp")
    q_copy = pltpu.make_async_copy(q_ref, q_hbm, sems.at[len(PIECES)])
    ends = [sum(PIECES[: n + 1]) for n in range(len(PIECES))]
    layers = tile_layers()
    q_new = (q_mine[...] + q_other[...]) * 0.5
    q_ref[...] = q_new
    q_copy.start()
    rounded = q_new.astype(BF16).astype(F32)
    zero = jnp.zeros((4, LANES), F32)
    for layer in range(len(SIZES)):
        q = rounded[layer]
        rows = (jnp.concatenate([q, zero], 1), jnp.concatenate([zero, q], 1))
        none = jnp.zeros((4, 2 * LANES), F32)
        weights[layer, 0] = jnp.concatenate([rows[0], none, rows[1], none], 0)
        weights[layer, 1] = jnp.concatenate([none, rows[0], none, rows[1]], 0)

    def copy(n):
        rows = pl.ds((ends[n] - PIECES[n]) * TILE, PIECES[n] * TILE)
        return pltpu.make_async_copy(obuf.at[rows], out_hbm.at[0, rows], sems.at[n])

    for n in range(TILES // GROUP):
        left = turned[n]
        for k in range(GROUP):
            t = n * GROUP + k
            for other in range(2):
                w = weights[layers[t], other].astype(BF16)
                parts = [w]
                if k:
                    parts.insert(0, jnp.zeros((16 * k, 2 * LANES), BF16))
                if k < GROUP - 1:
                    parts.append(jnp.zeros((LANES - 16 * (k + 1), 2 * LANES), BF16))
                update = jnp.dot(left, jnp.concatenate(parts, 0), preferred_element_type=F32)
                which = own if other == 0 else 1 - own
                at = pl.multiple_of(t * TILE + which * HALF, HALF)
                for h in range(2):
                    rows = pl.ds(pl.multiple_of(at + h * LANES, LANES), LANES)
                    obuf[rows] = (
                        comp[rows].astype(F32) - update[:, h * LANES : (h + 1) * LANES]
                    ).astype(BF16)
            if t + 1 in ends:
                copy(ends.index(t + 1)).start()
    q_copy.wait()
    for n in range(len(PIECES)):
        copy(n).wait()


def new_residual(q_mine, q_other, turned, comp):
    return pl.pallas_call(
        residual_kernel,
        out_shape=(
            jax.ShapeDtypeStruct((1, ROWS, LANES), BF16),
            jax.ShapeDtypeStruct((len(SIZES), 4, LANES), F32),
        ),
        in_specs=[VM, VM, VM, VM],
        out_specs=(HB, HB),
        scratch_shapes=[
            pltpu.VMEM((len(SIZES), 2, 16, 2 * LANES), F32),
            pltpu.VMEM((ROWS, LANES), BF16),
            pltpu.VMEM((len(SIZES), 4, LANES), F32),
            pltpu.SemaphoreType.DMA((len(PIECES) + 1,)),
        ],
        compiler_params=pltpu.CompilerParams(vmem_limit_bytes=24 * MIB),
        name="new_residual",
    )(q_mine, q_other, turned, comp)


def body(grad, residual, q_prev, owner_table):
    comp, keep, send, flags = project(grad, residual, q_prev, owner_table)
    both = keep + lax.ppermute(send, "grp", SWAP)
    arrived = lax.all_to_all(both, "dp", 0, 0, tiled=True)
    mine = lax.all_to_all(spread(arrived), "dp", 0, 0, tiled=True)
    other = lax.ppermute(mine, "grp", SWAP)
    q_part, stacked = orthonormal_bases(mine, other, comp)
    q_there = lax.ppermute(q_part, "grp", SWAP)
    turned, owned = aside(flags, mine, other, stacked)
    out, q_new = new_residual(q_part, q_there, turned, comp)
    return out, q_new, owned


def solution(mesh):
    in_specs = (P("grp", None, "dp"), P("grp", None, "dp"), P(None, None, "dp"), P())
    out_specs = (P("grp", None, "dp"), P(None, None, "dp"), P("dp", None, None))
    return jax.shard_map(body, mesh=mesh, in_specs=in_specs, out_specs=out_specs, check_vma=False)
```

```python
import functools

import jax
import jax.numpy as jnp
from jax import lax
from jax.experimental import pallas as pl
from jax.experimental.pallas import tpu as pltpu
from jax.sharding import PartitionSpec as P

D = 8192
KV = 1024
FF_WIN = 14336
SIZES = (D, KV, KV, D, FF_WIN)
ROWS = sum(SIZES)
LANES = 128
TILE = 512
HALF = TILE // 2
TILES = ROWS // TILE
GROUP = 8
EPSILON = 1e-06
SWAP = ((0, 1), (1, 0))
F32, BF16 = jnp.float32, jnp.bfloat16
MIB = 1 << 20


def tile_layers():
    return [layer for layer, rows in enumerate(SIZES) for _ in range(rows // TILE)]


def layer_starts():
    starts, at = [], 0
    for rows in SIZES:
        starts.append(at)
        at += rows // TILE
    return starts


VM = pl.BlockSpec(memory_space=pltpu.VMEM)
HB = pl.BlockSpec(memory_space=pltpu.HBM)


CHUNKS = (6, 14, 22, 12, 6, 4)
DEPTH = 3


def project_kernel(
    grad, residual, q_hbm, owner_hbm,
    comp_ref, keep_ref, send_ref, flags_ref,
    gbuf, rbuf, q_ref, lhs, owner, sems, q_sem, owner_sem,
):
    firsts = [sum(CHUNKS[:c]) for c in range(len(CHUNKS))]

    def copies(c):
        rows = pl.ds(firsts[c] * TILE, CHUNKS[c] * TILE)
        return (
            pltpu.make_async_copy(grad.at[0, rows], gbuf.at[rows], sems.at[0, c]),
            pltpu.make_async_copy(residual.at[0, rows], rbuf.at[rows], sems.at[1, c]),
        )

    q_copy = pltpu.make_async_copy(q_hbm, q_ref, q_sem)
    q_copy.start()
    owner_copy = pltpu.make_async_copy(owner_hbm, owner, owner_sem)
    owner_copy.start()
    for c in range(DEPTH):
        for copy in copies(c):
            copy.start()
    own = lax.axis_index("grp")
    q_copy.wait()
    for layer in range(len(SIZES)):
        q = q_ref[layer].astype(BF16).astype(F32)
        zero = jnp.zeros_like(q)
        straight = jnp.concatenate(
            [jnp.concatenate([q, zero], 1), jnp.concatenate([zero, q], 1)], 0
        )
        crossed = jnp.concatenate(
            [jnp.concatenate([zero, q], 1), jnp.concatenate([q, zero], 1)], 0
        )
        lhs[layer] = jnp.where(own == 0, straight, crossed)

    layers = tile_layers()
    for c, count in enumerate(CHUNKS):
        for copy in copies(c):
            copy.wait()
        if c + DEPTH < len(CHUNKS):
            for copy in copies(c + DEPTH):
                copy.start()
        if c == 1:
            owner_copy.wait()
            place = lax.axis_index("dp")
            for layer in range(len(SIZES)):
                held = jnp.where(owner[layer] == place, 1.0, 0.0)
                flags_ref[layer] = jnp.full((4, HALF), held, F32)
        for t in range(firsts[c], firsts[c] + count):
            halves = []
            for h in range(2):
                rows = slice(t * TILE + h * HALF, t * TILE + (h + 1) * HALF)
                value = (gbuf[rows].astype(F32) + rbuf[rows].astype(F32)).astype(BF16)
                comp_ref[rows] = value
                halves.append(value)
            out = lax.dot_general(
                lhs[layers[t]].astype(BF16),
                jnp.concatenate(halves, 1),
                (((1,), (1,)), ((), ())),
                preferred_element_type=F32,
            )
            keep_ref[t] = out[:4]
            send_ref[t] = out[4:]


def project(grad, residual, q_prev, owner_table):
    share = jax.ShapeDtypeStruct((TILES, 4, HALF), F32)
    return pl.pallas_call(
        project_kernel,
        out_shape=(
            pltpu.VMEM((ROWS, LANES), BF16),
            share,
            share,
            pltpu.VMEM((len(SIZES), 4, HALF), F32),
        ),
        in_specs=[HB, HB, HB, HB],
        out_specs=(VM, VM, VM, VM),
        scratch_shapes=[
            pltpu.VMEM((ROWS, LANES), BF16),
            pltpu.VMEM((ROWS, LANES), BF16),
            pltpu.VMEM((len(SIZES), 4, LANES), F32),
            pltpu.VMEM((len(SIZES), 8, 2 * LANES), F32),
            pltpu.SMEM((len(SIZES),), jnp.int32),
            pltpu.SemaphoreType.DMA((2, len(CHUNKS))),
            pltpu.SemaphoreType.DMA,
            pltpu.SemaphoreType.DMA,
        ],
        compiler_params=pltpu.CompilerParams(vmem_limit_bytes=30 * MIB),
        name="project",
    )(*(pltpu.with_memory_space_constraint(x, pltpu.HBM) for x in (grad, residual, q_prev, owner_table)))


def spread_kernel(x_ref, o_ref):
    total = x_ref[0]
    for i in range(1, TILES):
        total = total + x_ref[i]
    total = total * 0.5
    for i in range(TILES):
        o_ref[i] = total


def spread(x):
    return pl.pallas_call(
        spread_kernel,
        out_shape=jax.ShapeDtypeStruct((TILES, 4, HALF), F32),
        in_specs=[VM],
        out_specs=VM,
        compiler_params=pltpu.CompilerParams(vmem_limit_bytes=2 * MIB),
        name="spread",
    )(x)


def lane_sum(x):
    return jnp.sum(x, axis=1, keepdims=True)


def coefficients(grams):
    lane = lax.broadcasted_iota(jnp.int32, (8, LANES), 1)
    row = lax.broadcasted_iota(jnp.int32, (8, LANES), 0) % 4
    entry = {}
    for k in range(4):
        packed = jnp.zeros((8, LANES), F32)
        for layer, sums in enumerate(grams):
            s = sums[k][:, :LANES] + sums[k][:, LANES:]
            s = s + pltpu.roll(s, 4, 0)
            packed = jnp.where(lane == layer, lane_sum(s), packed)
        for i in range(k, 4):
            value = jnp.broadcast_to(packed[i : i + 1], (8, LANES))
            entry[i, i - k] = value + EPSILON if k == 0 else value
    g = entry
    i0 = lax.rsqrt(g[0, 0])
    l10, l20, l30 = g[1, 0] * i0, g[2, 0] * i0, g[3, 0] * i0
    i1 = lax.rsqrt(g[1, 1] - l10 * l10)
    l21 = (g[2, 1] - l20 * l10) * i1
    l31 = (g[3, 1] - l30 * l10) * i1
    i2 = lax.rsqrt(g[2, 2] - l20 * l20 - l21 * l21)
    l32 = (g[3, 2] - l30 * l20 - l31 * l21) * i2
    i3 = lax.rsqrt(g[3, 3] - l30 * l30 - l31 * l31 - l32 * l32)
    x = {(0, 0): i0, (1, 1): i1, (2, 2): i2, (3, 3): i3}
    x[1, 0] = -(l10 * i0) * i1
    x[2, 1] = -(l21 * i1) * i2
    x[3, 2] = -(l32 * i2) * i3
    x[2, 0] = -(l20 * i0 + l21 * x[1, 0]) * i2
    x[3, 1] = -(l31 * i1 + l32 * x[2, 1]) * i3
    x[3, 0] = -(l30 * i0 + l31 * x[1, 0] + l32 * x[2, 0]) * i3
    columns = []
    for k in range(4):
        packed = jnp.zeros((8, LANES), F32)
        for i in range(k, 4):
            packed = jnp.where(row == i, x[i, i - k], packed)
        columns.append(
            [
                jnp.broadcast_to(packed[:, layer : layer + 1], (8, 2 * LANES))
                for layer in range(len(grams))
            ]
        )
    return columns


EARLY, LATE = (0,), (4, 3, 1, 2)


def basis_kernel(mine, other, comp, q_ref, stacked, joined):
    own = lax.axis_index("grp")
    counts = [rows // TILE for rows in SIZES]
    starts = layer_starts()

    def gram(layer):
        sums = [None] * 4
        for t in range(starts[layer], starts[layer] + counts[layer]):
            v = jnp.concatenate([mine[t], other[t]], 0)
            joined[t] = v
            for k in range(4):
                term = v * (pltpu.roll(v, k, 0) if k else v)
                sums[k] = term if sums[k] is None else sums[k] + term
        return sums

    def apply(layer, columns):
        total = None
        for t in range(starts[layer], starts[layer] + counts[layer]):
            v = joined[t]
            basis = v * columns[0]
            for k in range(1, 4):
                basis = basis + pltpu.roll(v, k, 0) * columns[k]
            rounded = basis.astype(BF16)
            back = rounded.astype(F32)
            at = (t % GROUP) * 16
            stacked[t // GROUP, at : at + 8] = back[:, :LANES]
            stacked[t // GROUP, at + 8 : at + 16] = back[:, LANES:]
            first = comp[pl.ds(pl.multiple_of(t * TILE + own * HALF, HALF), HALF)]
            second = comp[pl.ds(pl.multiple_of(t * TILE + (1 - own) * HALF, HALF), HALF)]
            part = jnp.dot(
                rounded, jnp.concatenate([first, second], 1), preferred_element_type=F32
            )
            total = part if total is None else total + part
        q_ref[layer] = total[:4, :LANES] + total[4:, LANES:]

    early = coefficients([gram(layer) for layer in EARLY])
    late_grams = [gram(layer) for layer in LATE]
    for i, layer in enumerate(EARLY):
        apply(layer, [column[i] for column in early])
    late = coefficients(late_grams)
    for i, layer in enumerate(LATE):
        apply(layer, [column[i] for column in late])


def orthonormal_bases(mine, other, comp):
    return pl.pallas_call(
        basis_kernel,
        out_shape=(
            jax.ShapeDtypeStruct((len(SIZES), 4, LANES), F32),
            pltpu.VMEM((TILES // GROUP, LANES, LANES), F32),
        ),
        in_specs=[VM, VM, VM],
        out_specs=(VM, VM),
        scratch_shapes=[pltpu.VMEM((TILES, 8, HALF), F32)],
        compiler_params=pltpu.CompilerParams(vmem_limit_bytes=16 * MIB),
        name="bases",
    )(mine, other, comp)


def aside_kernel(flags, mine, other, stacked, turned_ref, owned_ref):
    own = lax.axis_index("grp")
    for n in range(TILES // GROUP):
        turned_ref[n] = stacked[n].T.astype(BF16)
    starts = layer_starts()
    counts = [rows // TILE for rows in SIZES]
    held = [flags[layer] > 0.5 for layer in range(len(SIZES))]
    for k in range(max(counts)):
        for ref, which in ((mine, own), (other, 1 - own)):
            value = jnp.zeros((4, HALF), F32)
            for layer, first in enumerate(starts):
                if k < counts[layer]:
                    value = jnp.where(held[layer], ref[first + k], value)
            owned_ref[0, :, pl.ds(pl.multiple_of(k * TILE + which * HALF, HALF), HALF)] = value


def aside(flags, mine, other, stacked):
    return pl.pallas_call(
        aside_kernel,
        out_shape=(
            pltpu.VMEM((TILES // GROUP, LANES, LANES), BF16),
            pltpu.VMEM((1, 4, max(SIZES)), F32),
        ),
        in_specs=[VM, VM, VM, VM],
        out_specs=(VM, VM),
        compiler_params=pltpu.CompilerParams(vmem_limit_bytes=4 * MIB),
        cost_estimate=pl.CostEstimate(flops=2_000_000, bytes_accessed=1_000_000, transcendentals=0),
        name="aside",
    )(flags, mine, other, stacked)


PIECES = (4,) * 16


def residual_kernel(
    q_mine, q_other, turned, comp, owned, out_hbm, q_hbm, owned_hbm, weights, obuf, q_ref, sems
):
    own = lax.axis_index("grp")
    owned_copy = pltpu.make_async_copy(owned, owned_hbm, sems.at[len(PIECES) + 1])
    owned_copy.start()
    q_copy = pltpu.make_async_copy(q_ref, q_hbm, sems.at[len(PIECES)])
    ends = [sum(PIECES[: n + 1]) for n in range(len(PIECES))]
    layers = tile_layers()
    q_new = (q_mine[...] + q_other[...]) * 0.5
    q_ref[...] = q_new
    q_copy.start()
    rounded = q_new.astype(BF16).astype(F32)
    zero = jnp.zeros((4, LANES), F32)
    for layer in range(len(SIZES)):
        q = rounded[layer]
        rows = (jnp.concatenate([q, zero], 1), jnp.concatenate([zero, q], 1))
        none = jnp.zeros((4, 2 * LANES), F32)
        weights[layer, 0] = jnp.concatenate([rows[0], none, rows[1], none], 0)
        weights[layer, 1] = jnp.concatenate([none, rows[0], none, rows[1]], 0)

    def copy(n):
        rows = pl.ds((ends[n] - PIECES[n]) * TILE, PIECES[n] * TILE)
        return pltpu.make_async_copy(obuf.at[rows], out_hbm.at[0, rows], sems.at[n])

    for n in range(TILES // GROUP):
        left = turned[n]
        for k in range(GROUP):
            t = n * GROUP + k
            for other in range(2):
                w = weights[layers[t], other].astype(BF16)
                parts = [w]
                if k:
                    parts.insert(0, jnp.zeros((16 * k, 2 * LANES), BF16))
                if k < GROUP - 1:
                    parts.append(jnp.zeros((LANES - 16 * (k + 1), 2 * LANES), BF16))
                update = jnp.dot(left, jnp.concatenate(parts, 0), preferred_element_type=F32)
                which = own if other == 0 else 1 - own
                at = pl.multiple_of(t * TILE + which * HALF, HALF)
                for h in range(2):
                    rows = pl.ds(pl.multiple_of(at + h * LANES, LANES), LANES)
                    obuf[rows] = (
                        comp[rows].astype(F32) - update[:, h * LANES : (h + 1) * LANES]
                    ).astype(BF16)
            if t + 1 in ends:
                copy(ends.index(t + 1)).start()
    owned_copy.wait()
    q_copy.wait()
    for n in range(len(PIECES)):
        copy(n).wait()


def new_residual(q_mine, q_other, turned, comp, owned):
    return pl.pallas_call(
        residual_kernel,
        out_shape=(
            jax.ShapeDtypeStruct((1, ROWS, LANES), BF16),
            jax.ShapeDtypeStruct((len(SIZES), 4, LANES), F32),
            jax.ShapeDtypeStruct((1, 4, max(SIZES)), F32),
        ),
        in_specs=[VM, VM, VM, VM, VM],
        out_specs=(HB, HB, HB),
        scratch_shapes=[
            pltpu.VMEM((len(SIZES), 2, 16, 2 * LANES), F32),
            pltpu.VMEM((ROWS, LANES), BF16),
            pltpu.VMEM((len(SIZES), 4, LANES), F32),
            pltpu.SemaphoreType.DMA((len(PIECES) + 2,)),
        ],
        compiler_params=pltpu.CompilerParams(vmem_limit_bytes=24 * MIB),
        name="new_residual",
    )(q_mine, q_other, turned, comp, owned)


def body(grad, residual, q_prev, owner_table):
    comp, keep, send, flags = project(grad, residual, q_prev, owner_table)
    both = keep + lax.ppermute(send, "grp", SWAP)
    arrived = lax.all_to_all(both, "dp", 0, 0, tiled=True)
    mine = lax.all_to_all(spread(arrived), "dp", 0, 0, tiled=True)
    other = lax.ppermute(mine, "grp", SWAP)
    q_part, stacked = orthonormal_bases(mine, other, comp)
    q_there = lax.ppermute(q_part, "grp", SWAP)
    turned, owned = aside(flags, mine, other, stacked)
    return new_residual(q_part, q_there, turned, comp, owned)


def solution(mesh):
    in_specs = (P("grp", None, "dp"), P("grp", None, "dp"), P(None, None, "dp"), P())
    out_specs = (P("grp", None, "dp"), P(None, None, "dp"), P("dp", None, None))
    return jax.shard_map(body, mesh=mesh, in_specs=in_specs, out_specs=out_specs, check_vma=False)
```

```python
import functools

import jax
import jax.numpy as jnp
from jax import lax
from jax.experimental import pallas as pl
from jax.experimental.pallas import tpu as pltpu
from jax.sharding import PartitionSpec as P

D = 8192
KV = 1024
FF_WIN = 14336
SIZES = (D, KV, KV, D, FF_WIN)
ROWS = sum(SIZES)
LANES = 128
TILE = 512
HALF = TILE // 2
TILES = ROWS // TILE
GROUP = 8
EPSILON = 1e-06
SWAP = ((0, 1), (1, 0))
F32, BF16 = jnp.float32, jnp.bfloat16
MIB = 1 << 20


def tile_layers():
    return [layer for layer, rows in enumerate(SIZES) for _ in range(rows // TILE)]


def layer_starts():
    starts, at = [], 0
    for rows in SIZES:
        starts.append(at)
        at += rows // TILE
    return starts


VM = pl.BlockSpec(memory_space=pltpu.VMEM)
HB = pl.BlockSpec(memory_space=pltpu.HBM)


CHUNKS = (6, 14, 22, 12, 6, 4)
DEPTH = 3


def project_kernel(
    grad, residual, q_hbm, owner_hbm,
    comp_ref, keep_ref, send_ref, flags_ref,
    gbuf, rbuf, q_ref, lhs, owner, sems, q_sem, owner_sem,
):
    firsts = [sum(CHUNKS[:c]) for c in range(len(CHUNKS))]

    def copies(c):
        rows = pl.ds(firsts[c] * TILE, CHUNKS[c] * TILE)
        return (
            pltpu.make_async_copy(grad.at[0, rows], gbuf.at[rows], sems.at[0, c]),
            pltpu.make_async_copy(residual.at[0, rows], rbuf.at[rows], sems.at[1, c]),
        )

    q_copy = pltpu.make_async_copy(q_hbm, q_ref, q_sem)
    q_copy.start()
    owner_copy = pltpu.make_async_copy(owner_hbm, owner, owner_sem)
    owner_copy.start()
    for c in range(DEPTH):
        for copy in copies(c):
            copy.start()
    own = lax.axis_index("grp")
    q_copy.wait()
    for layer in range(len(SIZES)):
        q = q_ref[layer].astype(BF16).astype(F32)
        zero = jnp.zeros_like(q)
        straight = jnp.concatenate(
            [jnp.concatenate([q, zero], 1), jnp.concatenate([zero, q], 1)], 0
        )
        crossed = jnp.concatenate(
            [jnp.concatenate([zero, q], 1), jnp.concatenate([q, zero], 1)], 0
        )
        lhs[layer] = jnp.where(own == 0, straight, crossed)

    layers = tile_layers()
    for c, count in enumerate(CHUNKS):
        for copy in copies(c):
            copy.wait()
        if c + DEPTH < len(CHUNKS):
            for copy in copies(c + DEPTH):
                copy.start()
        if c == 1:
            owner_copy.wait()
            place = lax.axis_index("dp")
            for layer in range(len(SIZES)):
                held = jnp.where(owner[layer] == place, 1.0, 0.0)
                flags_ref[layer] = jnp.full((4, HALF), held, F32)
        for t in range(firsts[c], firsts[c] + count):
            halves = []
            for h in range(2):
                rows = slice(t * TILE + h * HALF, t * TILE + (h + 1) * HALF)
                value = (gbuf[rows].astype(F32) + rbuf[rows].astype(F32)).astype(BF16)
                comp_ref[rows] = value
                halves.append(value)
            out = lax.dot_general(
                lhs[layers[t]].astype(BF16),
                jnp.concatenate(halves, 1),
                (((1,), (1,)), ((), ())),
                preferred_element_type=F32,
            )
            keep_ref[t] = out[:4]
            send_ref[t] = out[4:]


def project(grad, residual, q_prev, owner_table):
    share = jax.ShapeDtypeStruct((TILES, 4, HALF), F32)
    return pl.pallas_call(
        project_kernel,
        out_shape=(
            pltpu.VMEM((ROWS, LANES), BF16),
            share,
            share,
            pltpu.VMEM((len(SIZES), 4, HALF), F32),
        ),
        in_specs=[HB, HB, HB, HB],
        out_specs=(VM, VM, VM, VM),
        scratch_shapes=[
            pltpu.VMEM((ROWS, LANES), BF16),
            pltpu.VMEM((ROWS, LANES), BF16),
            pltpu.VMEM((len(SIZES), 4, LANES), F32),
            pltpu.VMEM((len(SIZES), 8, 2 * LANES), F32),
            pltpu.SMEM((len(SIZES),), jnp.int32),
            pltpu.SemaphoreType.DMA((2, len(CHUNKS))),
            pltpu.SemaphoreType.DMA,
            pltpu.SemaphoreType.DMA,
        ],
        compiler_params=pltpu.CompilerParams(vmem_limit_bytes=30 * MIB),
        name="project",
    )(*(pltpu.with_memory_space_constraint(x, pltpu.HBM) for x in (grad, residual, q_prev, owner_table)))


def spread_kernel(x_ref, o_ref):
    total = x_ref[0]
    for i in range(1, TILES):
        total = total + x_ref[i]
    total = total * 0.5
    for i in range(TILES):
        o_ref[i] = total


def spread(x):
    return pl.pallas_call(
        spread_kernel,
        out_shape=jax.ShapeDtypeStruct((TILES, 4, HALF), F32),
        in_specs=[VM],
        out_specs=VM,
        compiler_params=pltpu.CompilerParams(vmem_limit_bytes=2 * MIB),
        name="spread",
    )(x)


def lane_sum(x):
    return jnp.sum(x, axis=1, keepdims=True)


def coefficients(grams):
    lane = lax.broadcasted_iota(jnp.int32, (8, LANES), 1)
    row = lax.broadcasted_iota(jnp.int32, (8, LANES), 0) % 4
    entry = {}
    for k in range(4):
        packed = jnp.zeros((8, LANES), F32)
        for layer, sums in enumerate(grams):
            s = sums[k][:, :LANES] + sums[k][:, LANES:]
            s = s + pltpu.roll(s, 4, 0)
            packed = jnp.where(lane == layer, lane_sum(s), packed)
        for i in range(k, 4):
            value = jnp.broadcast_to(packed[i : i + 1], (8, LANES))
            entry[i, i - k] = value + EPSILON if k == 0 else value
    g = entry
    i0 = lax.rsqrt(g[0, 0])
    l10, l20, l30 = g[1, 0] * i0, g[2, 0] * i0, g[3, 0] * i0
    i1 = lax.rsqrt(g[1, 1] - l10 * l10)
    l21 = (g[2, 1] - l20 * l10) * i1
    l31 = (g[3, 1] - l30 * l10) * i1
    i2 = lax.rsqrt(g[2, 2] - l20 * l20 - l21 * l21)
    l32 = (g[3, 2] - l30 * l20 - l31 * l21) * i2
    i3 = lax.rsqrt(g[3, 3] - l30 * l30 - l31 * l31 - l32 * l32)
    x = {(0, 0): i0, (1, 1): i1, (2, 2): i2, (3, 3): i3}
    x[1, 0] = -(l10 * i0) * i1
    x[2, 1] = -(l21 * i1) * i2
    x[3, 2] = -(l32 * i2) * i3
    x[2, 0] = -(l20 * i0 + l21 * x[1, 0]) * i2
    x[3, 1] = -(l31 * i1 + l32 * x[2, 1]) * i3
    x[3, 0] = -(l30 * i0 + l31 * x[1, 0] + l32 * x[2, 0]) * i3
    columns = []
    for k in range(4):
        packed = jnp.zeros((8, LANES), F32)
        for i in range(k, 4):
            packed = jnp.where(row == i, x[i, i - k], packed)
        columns.append(
            [
                jnp.broadcast_to(packed[:, layer : layer + 1], (8, 2 * LANES))
                for layer in range(len(grams))
            ]
        )
    return columns


EARLY, LATE = (0,), (4, 3, 1, 2)


def basis_kernel(mine, other, comp, q_ref, stacked, joined):
    own = lax.axis_index("grp")
    counts = [rows // TILE for rows in SIZES]
    starts = layer_starts()

    def gram(layer):
        sums = [None] * 4
        for t in range(starts[layer], starts[layer] + counts[layer]):
            v = jnp.concatenate([mine[t], other[t]], 0)
            joined[t] = v
            for k in range(4):
                term = v * (pltpu.roll(v, k, 0) if k else v)
                sums[k] = term if sums[k] is None else sums[k] + term
        return sums

    def apply(layer, columns):
        total = None
        for t in range(starts[layer], starts[layer] + counts[layer]):
            v = joined[t]
            basis = v * columns[0]
            for k in range(1, 4):
                basis = basis + pltpu.roll(v, k, 0) * columns[k]
            rounded = basis.astype(BF16)
            back = rounded.astype(F32)
            at = (t % GROUP) * 16
            stacked[t // GROUP, at : at + 8] = back[:, :LANES]
            stacked[t // GROUP, at + 8 : at + 16] = back[:, LANES:]
            first = comp[pl.ds(pl.multiple_of(t * TILE + own * HALF, HALF), HALF)]
            second = comp[pl.ds(pl.multiple_of(t * TILE + (1 - own) * HALF, HALF), HALF)]
            part = jnp.dot(
                rounded, jnp.concatenate([first, second], 1), preferred_element_type=F32
            )
            total = part if total is None else total + part
        q_ref[layer] = total[:4, :LANES] + total[4:, LANES:]

    early = coefficients([gram(layer) for layer in EARLY])
    late_grams = [gram(layer) for layer in LATE]
    for i, layer in enumerate(EARLY):
        apply(layer, [column[i] for column in early])
    late = coefficients(late_grams)
    for i, layer in enumerate(LATE):
        apply(layer, [column[i] for column in late])


def orthonormal_bases(mine, other, comp):
    return pl.pallas_call(
        basis_kernel,
        out_shape=(
            jax.ShapeDtypeStruct((len(SIZES), 4, LANES), F32),
            pltpu.VMEM((TILES // GROUP, LANES, LANES), F32),
        ),
        in_specs=[VM, VM, VM],
        out_specs=(VM, VM),
        scratch_shapes=[pltpu.VMEM((TILES, 8, HALF), F32)],
        compiler_params=pltpu.CompilerParams(vmem_limit_bytes=16 * MIB),
        name="bases",
    )(mine, other, comp)


def aside_kernel(flags, mine, other, stacked, turned_ref, owned_ref):
    own = lax.axis_index("grp")
    for n in range(TILES // GROUP):
        turned_ref[n] = stacked[n].T.astype(BF16)
    starts = layer_starts()
    counts = [rows // TILE for rows in SIZES]
    held = [flags[layer] > 0.5 for layer in range(len(SIZES))]
    for k in range(max(counts)):
        for ref, which in ((mine, own), (other, 1 - own)):
            value = jnp.zeros((4, HALF), F32)
            for layer, first in enumerate(starts):
                if k < counts[layer]:
                    value = jnp.where(held[layer], ref[first + k], value)
            owned_ref[0, :, pl.ds(pl.multiple_of(k * TILE + which * HALF, HALF), HALF)] = value


def aside(flags, mine, other, stacked):
    return pl.pallas_call(
        aside_kernel,
        out_shape=(
            pltpu.VMEM((TILES // GROUP, LANES, LANES), BF16),
            pltpu.VMEM((1, 4, max(SIZES)), F32),
        ),
        in_specs=[VM, VM, VM, VM],
        out_specs=(VM, VM),
        compiler_params=pltpu.CompilerParams(vmem_limit_bytes=4 * MIB),
        cost_estimate=pl.CostEstimate(flops=2_000_000, bytes_accessed=1_000_000, transcendentals=0),
        name="aside",
    )(flags, mine, other, stacked)


PIECES = (4,) * 16


def residual_kernel(
    q_mine, q_other, turned, comp, owned, out_hbm, q_hbm, owned_hbm, weights, obuf, q_ref, sems
):
    own = lax.axis_index("grp")
    owned_copy = pltpu.make_async_copy(owned, owned_hbm, sems.at[len(PIECES) + 1])
    owned_copy.start()
    q_copy = pltpu.make_async_copy(q_ref, q_hbm, sems.at[len(PIECES)])
    ends = [sum(PIECES[: n + 1]) for n in range(len(PIECES))]
    layers = tile_layers()
    q_new = (q_mine[...] + q_other[...]) * 0.5
    q_ref[...] = q_new
    q_copy.start()
    rounded = q_new.astype(BF16).astype(F32)
    zero = jnp.zeros((4, LANES), F32)
    for layer in range(len(SIZES)):
        q = rounded[layer]
        rows = (jnp.concatenate([q, zero], 1), jnp.concatenate([zero, q], 1))
        none = jnp.zeros((4, 2 * LANES), F32)
        weights[layer, 0] = jnp.concatenate([rows[0], none, rows[1], none], 0)
        weights[layer, 1] = jnp.concatenate([none, rows[0], none, rows[1]], 0)

    def copy(n):
        rows = pl.ds((ends[n] - PIECES[n]) * TILE, PIECES[n] * TILE)
        return pltpu.make_async_copy(obuf.at[rows], out_hbm.at[0, rows], sems.at[n])

    for n in range(TILES // GROUP):
        left = turned[n]
        for k in range(GROUP):
            t = n * GROUP + k
            for other in range(2):
                w = weights[layers[t], other].astype(BF16)
                parts = [w]
                if k:
                    parts.insert(0, jnp.zeros((16 * k, 2 * LANES), BF16))
                if k < GROUP - 1:
                    parts.append(jnp.zeros((LANES - 16 * (k + 1), 2 * LANES), BF16))
                update = jnp.dot(left, jnp.concatenate(parts, 0), preferred_element_type=F32)
                which = own if other == 0 else 1 - own
                at = pl.multiple_of(t * TILE + which * HALF, HALF)
                for h in range(2):
                    rows = pl.ds(pl.multiple_of(at + h * LANES, LANES), LANES)
                    obuf[rows] = (
                        comp[rows].astype(F32) - update[:, h * LANES : (h + 1) * LANES]
                    ).astype(BF16)
            if t + 1 in ends:
                copy(ends.index(t + 1)).start(priority=ends.index(t + 1) % 2)
    owned_copy.wait()
    q_copy.wait()
    for n in range(len(PIECES)):
        copy(n).wait()


def new_residual(q_mine, q_other, turned, comp, owned):
    return pl.pallas_call(
        residual_kernel,
        out_shape=(
            jax.ShapeDtypeStruct((1, ROWS, LANES), BF16),
            jax.ShapeDtypeStruct((len(SIZES), 4, LANES), F32),
            jax.ShapeDtypeStruct((1, 4, max(SIZES)), F32),
        ),
        in_specs=[VM, VM, VM, VM, VM],
        out_specs=(HB, HB, HB),
        scratch_shapes=[
            pltpu.VMEM((len(SIZES), 2, 16, 2 * LANES), F32),
            pltpu.VMEM((ROWS, LANES), BF16),
            pltpu.VMEM((len(SIZES), 4, LANES), F32),
            pltpu.SemaphoreType.DMA((len(PIECES) + 2,)),
        ],
        compiler_params=pltpu.CompilerParams(vmem_limit_bytes=24 * MIB),
        name="new_residual",
    )(q_mine, q_other, turned, comp, owned)


def body(grad, residual, q_prev, owner_table):
    comp, keep, send, flags = project(grad, residual, q_prev, owner_table)
    both = keep + lax.ppermute(send, "grp", SWAP)
    arrived = lax.all_to_all(both, "dp", 0, 0, tiled=True)
    mine = lax.all_to_all(spread(arrived), "dp", 0, 0, tiled=True)
    other = lax.ppermute(mine, "grp", SWAP)
    q_part, stacked = orthonormal_bases(mine, other, comp)
    q_there = lax.ppermute(q_part, "grp", SWAP)
    turned, owned = aside(flags, mine, other, stacked)
    return new_residual(q_part, q_there, turned, comp, owned)


def solution(mesh):
    in_specs = (P("grp", None, "dp"), P("grp", None, "dp"), P(None, None, "dp"), P())
    out_specs = (P("grp", None, "dp"), P(None, None, "dp"), P("dp", None, None))
    return jax.shard_map(body, mesh=mesh, in_specs=in_specs, out_specs=out_specs, check_vma=False)
```
